32 devices in a mesh: rows: 4 (over z), width: 4 (over y, x), site: 2 (over core).
Axes of the slice: x: 2, y: 2, z: 4, core: 2. Of those that a mesh axis runs over, the one named last changes fastest.
Arguments:
- weight_query: float32 [8192, 4096], P(('site', 'rows'), 'width'), parts along dimension 0, may hold values from -0.125 to 0.125
- moment_query: float32 [8192, 4096], P(('site', 'rows'), 'width'), parts along dimension 0, may hold values from -6 to 6
- square_query: float32 [8192, 4096], P(('site', 'rows'), 'width'), parts along dimension 0, may hold values from 0.1 to 10
- weight_key: float32 [8192, 1024], P(('site', 'rows'), 'width'), parts along dimension 0, may hold values from -0.125 to 0.125
- moment_key: float32 [8192, 1024], P(('site', 'rows'), 'width'), parts along dimension 0, may hold values from -6 to 6
- square_key: float32 [8192, 1024], P(('site', 'rows'), 'width'), parts along dimension 0, may hold values from 0.1 to 10
- weight_value: float32 [8192, 1024], P(('site', 'rows'), 'width'), parts along dimension 0, may hold values from -0.125 to 0.125
- moment_value: float32 [8192, 1024], P(('site', 'rows'), 'width'), parts along dimension 0, may hold values from -6 to 6
- square_value: float32 [8192, 1024], P(('site', 'rows'), 'width'), parts along dimension 0, may hold values from 0.1 to 10
- norm_train: float32 [8192], P(('site', 'rows', 'width')), parts along dimension 0, may hold values from 0.25 to 1.75
- norm_step: float32 [8192], P(('site', 'rows', 'width')), parts along dimension 0, may hold values from -0.3 to 0.3
Outputs:
- final_query: bfloat16 [8192, 4096], P('site', 'width'), parts along dimension 0
- final_key: bfloat16 [8192, 1024], P('site', 'width'), parts along dimension 0
- final_value: bfloat16 [8192, 1024], P('site', 'width'), parts along dimension 0
- column_query: float32 [8192], P(('site', 'width')), parts along dimension 0
- column_key: float32 [2048], P(('site', 'width')), parts along dimension 0
- column_value: float32 [2048], P(('site', 'width')), parts along dimension 0
- serve_norm: bfloat16 [8192], P('site'), parts along dimension 0
- result_query: float32 [8192, 4096], P(('site', 'rows'), 'width'), parts along dimension 0
- result_key: float32 [8192, 1024], P(('site', 'rows'), 'width'), parts along dimension 0
- result_value: float32 [8192, 1024], P(('site', 'rows'), 'width'), parts along dimension 0
The draws below stay inside these ranges and needn't reach their ends.
There are 2 independent parts, one for each index of `site`. The reference program is written for one: setup_inputs(seed, part) draws one part's arguments, and reference() takes and returns one part's arrays. A program takes and returns all parts, laid end to end along the dimension named above; each array names one. Nothing has to cross between parts.
All inputs are finite; a program needn't handle non-finite values.
Results may differ from the reference program's by a relative error of at most 0.001.
Values may be sent and summed in bfloat16 or wider, within the bound.
A program may use at most 128 MiB of HBM per device.

```python
import math
import jax
import jax.numpy as jnp
from jax import lax

D_MODEL = 4096
Q_DIM = 4096
KV_DIM = 1024


def strengthened(values, rng, source, target, parts, factor):
    def block_of(axis_at):
        return (jnp.arange(values.shape[axis_at]) // (values.shape[axis_at] // parts)).reshape((-1,) + (1,) * (values.ndim - 1 - axis_at))

    near = jax.random.permutation(rng, parts)[block_of(target)]
    far = (block_of(target) + parts // 2) % parts
    return jnp.where((block_of(source) == near) | (block_of(source) == far), factor * values, values)


def shard_levels(rng, shape, split, low, high):
    gain, own = 1.0, jax.random.fold_in(rng, 6)
    for dim, parts in split:
        draws = jnp.exp(jax.random.uniform(jax.random.fold_in(own, dim), (parts,), jnp.float32, low / len(split), high / len(split)))
        gain = gain * jnp.repeat(draws, shape[dim] // parts).reshape([-1 if axis == dim else 1 for axis in range(len(shape))])
    return gain


def bell_draw(key, dims, spread, reach, split=(), kind=jnp.bfloat16):
    loudness = shard_levels(key, dims, split, -0.22, 0.18) if split else 1.0
    result = jax.random.normal(key, dims, jnp.float32) * spread * loudness
    return jnp.minimum(jnp.maximum(result, -reach), reach).astype(kind)


def gaussian_with(rng, dims, width, bound, pieces, heavy, held_as=jnp.bfloat16):
    drawn = width * jax.random.normal(rng, dims, jnp.float32)
    if pieces:
        drawn = drawn * shard_levels(rng, dims, pieces, -0.22, 0.18)
    return jnp.clip(strengthened(drawn, jax.random.fold_in(rng, 3), *heavy), -bound, bound).astype(held_as)


def setup_inputs(seed: int = 0, part: int = 0) -> dict:
    key_of = jax.random.split(jax.random.key(seed), 12)
    own_keys = jax.random.split(jax.random.fold_in(key_of[11], part), 12)
    weight_query = gaussian_with(own_keys[0], (D_MODEL, Q_DIM), D_MODEL ** -0.5, 0.125, ((0, 4), (1, 4)), (0, 1, 4, 2.0), jnp.float32)
    moment_query = bell_draw(own_keys[1], (D_MODEL, Q_DIM), 1.0, 6.0, ((0, 4), (1, 4)), jnp.float32)
    square_query = jnp.clip(jnp.exp(math.log(10.0) - 4.6051702 * jax.random.uniform(own_keys[2], (D_MODEL, Q_DIM), jnp.float32) ** shard_levels(own_keys[2], (D_MODEL, Q_DIM), ((0, 4), (1, 4)), -0.2, 0.2)), 0.1, 10.0)
    weight_key = gaussian_with(own_keys[3], (D_MODEL, KV_DIM), D_MODEL ** -0.5, 0.125, ((0, 4), (1, 4)), (0, 1, 4, 2.0), jnp.float32)
    moment_key = bell_draw(own_keys[4], (D_MODEL, KV_DIM), 1.0, 6.0, ((0, 4), (1, 4)), jnp.float32)
    square_key = jnp.clip(jnp.exp(math.log(10.0) - 4.6051702 * jax.random.uniform(own_keys[5], (D_MODEL, KV_DIM), jnp.float32) ** shard_levels(own_keys[5], (D_MODEL, KV_DIM), ((0, 4), (1, 4)), -0.2, 0.2)), 0.1, 10.0)
    weight_value = gaussian_with(own_keys[6], (D_MODEL, KV_DIM), D_MODEL ** -0.5, 0.125, ((0, 4), (1, 4)), (0, 1, 4, 2.0), jnp.float32)
    moment_value = bell_draw(own_keys[7], (D_MODEL, KV_DIM), 1.0, 6.0, ((0, 4), (1, 4)), jnp.float32)
    square_value = jnp.clip(jnp.exp(math.log(10.0) - 4.6051702 * jax.random.uniform(own_keys[8], (D_MODEL, KV_DIM), jnp.float32) ** shard_levels(own_keys[8], (D_MODEL, KV_DIM), ((0, 4), (1, 4)), -0.2, 0.2)), 0.1, 10.0)
    norm_train = jnp.clip(1.0 + 0.15 * jax.random.normal(own_keys[9], (D_MODEL,), jnp.float32), 0.25, 1.75)
    norm_step = jnp.clip(jax.random.uniform(own_keys[10], (D_MODEL,), jnp.float32, -0.3, 0.3) * shard_levels(own_keys[10], (D_MODEL,), ((0, 16),), -0.4, 0.0), -0.3, 0.3)
    return dict(weight_query=weight_query, moment_query=moment_query, square_query=square_query, weight_key=weight_key, moment_key=moment_key, square_key=square_key, weight_value=weight_value, moment_value=moment_value, square_value=square_value, norm_train=norm_train, norm_step=norm_step)


learn_rate = 0.02
decay_rate = 0.05
tiny_value = 1e-08

def reference(weight_query, moment_query, square_query, weight_key, moment_key, square_key, weight_value, moment_value, square_value, norm_train, norm_step):
    result_query = weight_query - learn_rate * (moment_query / (jnp.sqrt(square_query) + tiny_value) + decay_rate * weight_query)
    result_key = weight_key - learn_rate * (moment_key / (jnp.sqrt(square_key) + tiny_value) + decay_rate * weight_key)
    result_value = weight_value - learn_rate * (moment_value / (jnp.sqrt(square_value) + tiny_value) + decay_rate * weight_value)
    column_query = jnp.sqrt(lax.optimization_barrier(jnp.sum(result_query * result_query, axis=0)))
    final_query = (result_query / column_query).astype(jnp.bfloat16)
    column_key = jnp.sqrt(lax.optimization_barrier(jnp.sum(result_key * result_key, axis=0)))
    final_key = (result_key / column_key).astype(jnp.bfloat16)
    column_value = jnp.sqrt(lax.optimization_barrier(jnp.sum(result_value * result_value, axis=0)))
    final_value = (result_value / column_value).astype(jnp.bfloat16)
    serve_norm = (norm_train + norm_step).astype(jnp.bfloat16)
    return (final_query, final_key, final_value, column_query, column_key, column_value, serve_norm, result_query, result_key, result_value)
```

```python
import functools

import jax
import jax.numpy as jnp
from jax import lax
from jax.experimental import pallas as pl
from jax.experimental.pallas import tpu as pltpu
from jax.sharding import PartitionSpec as P

learn_rate = 0.02
decay_rate = 0.05
tiny_value = 1e-08

LAG = 1
HELD = 4, 8
MESH = pl.DeviceIdType.MESH


def chunks_of(widths):
    out = []
    for a, width in enumerate(widths):
        step = 128 if width % 128 == 0 else width
        out += [(a, c, step) for c in range(0, width, step)]
    return out


def late_of(chunks):
    count = sum(1 for ch in chunks if ch[0] == 0)
    return count - max(1, count * HELD[0] // HELD[1])


def waits(n, site):
    me = lax.axis_index("rows")
    late = lax.axis_index("site") == site - 1
    return me, late & (me == 0), late & (me == n - 1)


def gather(n, site, chunks, *refs):
    inputs, norms = [refs[0:3], refs[3:6], refs[6:9]], refs[9:11]
    finals, columns, gains, results = refs[11:14], refs[14:17], refs[17], refs[18:21]
    held = [refs[21:24], refs[24:27], refs[27:30]]
    gain, sums, in_sem, gain_sem, sum_send, sum_recv, send, recv, norm_send, norm_recv = refs[30:]
    me, first, last = waits(n, site)
    late = lax.axis_index("site") == site - 1
    depth = results[0].shape[0]
    block = min(depth, 64)
    split = late_of(chunks)
    counts = [sum(1 for ch in chunks if ch[0] == a) for a in range(3)]
    bases = [sum(counts[:a]) for a in range(3)]

    barrier = pltpu.get_barrier_semaphore()

    def load(j, k):
        a, c, cw = chunks[j]
        return pltpu.make_async_copy(
            inputs[a][k].at[:, pl.ds(c, cw)], held[a][k].at[:, pl.ds(c, cw)], in_sem.at[j, k]
        )

    for p in range(1, n):
        pl.semaphore_signal(
            barrier, inc=1, device_id={"rows": lax.rem(me + p, n)}, device_id_type=MESH
        )
    ahead = min(2, len(chunks))
    for j in range(ahead):
        for k in range(3):
            load(j, k).start()
    for k in range(2):
        pltpu.make_async_copy(norms[k], gain.at[k], gain_sem.at[k]).start()

    def update(j):
        a, c, cw = chunks[j]
        for k in range(3):
            load(j, k).wait()
        if j + ahead < len(chunks):
            for k in range(3):
                load(j + ahead, k).start()
        weight, moment, square = held[a]
        cols = pl.ds(c, cw)

        def body(i, acc):
            rows = pl.ds(pl.multiple_of(i * block, block), block)
            w = weight[rows, cols]
            r = w - learn_rate * (
                moment[rows, cols] / (jnp.sqrt(square[rows, cols]) + tiny_value) + decay_rate * w
            )
            results[a][rows, cols] = r
            return acc + jnp.sum((r * r).reshape(block // 8, 8, cw), axis=0)

        acc = lax.fori_loop(0, depth // block, body, jnp.zeros((8, cw), jnp.float32))
        sums[j, me, :, pl.ds(0, cw)] = jnp.sum(acc, axis=0, keepdims=True)

    def sum_copy(j, p, slot):
        return pltpu.make_async_remote_copy(
            src_ref=sums.at[j, me], dst_ref=sums.at[j, slot],
            send_sem=sum_send.at[j, p], recv_sem=sum_recv.at[j, p],
            device_id={"rows": lax.rem(me + p, n)}, device_id_type=MESH,
        )

    def norm_copy(p, slot):
        return pltpu.make_async_remote_copy(
            src_ref=gains.at[me], dst_ref=gains.at[slot],
            send_sem=norm_send.at[p], recv_sem=norm_recv.at[p],
            device_id={"rows": lax.rem(me + p, n)}, device_id_type=MESH,
        )

    has_next = (me < n - 1, me > 0)
    step = (1, -1)
    keeps = (late & (me == n - 2), late & (me == 1))
    lacks = (last, first)

    def pass_on(d, h, j, a, cols, origin):
        rows = pl.ds(pl.multiple_of(origin * depth, depth), depth)
        return pltpu.make_async_remote_copy(
            src_ref=finals[a].at[rows, cols], dst_ref=finals[a].at[rows, cols],
            send_sem=send.at[d, h, j], recv_sem=recv.at[d, h, j],
            device_id={"rows": lax.rem(me + step[d] + n, n)}, device_id_type=MESH,
        )

    def finish(j):
        a, c, cw = chunks[j]
        cols = pl.ds(c, cw)
        for p in range(1, n):
            sum_copy(j, p, lax.rem(me - p + n, n)).wait_recv()
        total = sums[j, 0, :, pl.ds(0, cw)]
        for p in range(1, n):
            total = total + sums[j, p, :, pl.ds(0, cw)]
        scale = jnp.sqrt(total)
        columns[a][:, cols] = scale
        inverse = 1.0 / scale

        def body(i, carry):
            rows = pl.ds(pl.multiple_of(i * block, block), block)
            mine = pl.ds(pl.multiple_of(me * depth + i * block, block), block)
            finals[a][mine, cols] = (results[a][rows, cols] * inverse).astype(jnp.bfloat16)
            return carry

        lax.fori_loop(0, depth // block, body, 0)
        for d in (0, 1):
            goes = has_next[d]
            if a == 0 and j >= split:
                goes = goes & jnp.logical_not(keeps[d])

            @pl.when(goes)
            def _(d=d):
                pass_on(d, 0, j, a, cols, me).start()

    for j in range(len(chunks) + LAG):
        if j < len(chunks):
            update(j)
            if j == 0:
                pl.semaphore_wait(barrier, n - 1)
            for p in range(1, n):
                sum_copy(j, p, me).start()
        if j >= LAG:
            finish(j - LAG)

    for k in range(2):
        pltpu.make_async_copy(norms[k], gain.at[k], gain_sem.at[k]).wait()
    gains[me] = (gain[0] + gain[1]).astype(jnp.bfloat16)
    for p in range(1, n):
        norm_copy(p, me).start()

    def span(a, cut, visit):
        cw = chunks[bases[a]][2]

        def body(k, carry):
            start = pl.multiple_of(k * cw, 128) if counts[a] > 1 else 0
            visit(bases[a] + k, a, pl.ds(start, cw))
            return carry

        low, high = cut
        if counts[a] > 1:
            lax.fori_loop(low, high, body, 0)
        elif high > low:
            body(0, 0)

    def parts(a, h):
        if a == 0 and h == 0:
            return ((0, split), False), ((split, counts[0]), True)
        return (((0, counts[a]), False),)

    def relay(h):
        for a in range(3):
            for cut, tail in parts(a, h):

                def visit(j, a, cols, tail=tail):
                    for d in (0, 1):
                        origin = me - step[d] * (h + 1)
                        comes = (origin >= 0) & (origin < n)
                        if tail:
                            comes = comes & jnp.logical_not(lacks[d])

                        @pl.when(comes)
                        def _(d=d, origin=origin):
                            pass_on(d, h, j, a, cols, origin).wait_recv()

                            if h + 1 < n - 1:
                                @pl.when(has_next[d])
                                def _():
                                    pass_on(d, h + 1, j, a, cols, origin).start()

                span(a, cut, visit)

    def drain(h):
        for d in (0, 1):
            origin = me - step[d] * h
            for a in range(3):
                for cut, tail in parts(a, h):
                    went = has_next[d] & (origin >= 0) & (origin < n)
                    if tail:
                        went = went & jnp.logical_not(keeps[d])

                    @pl.when(went)
                    def _(d=d, a=a, cut=cut, origin=origin):
                        span(
                            a, cut,
                            lambda j, a, cols: pass_on(d, h, j, a, cols, origin).wait_send(),
                        )

    for h in range(n - 1):
        if h == n - 2:
            for j in range(len(chunks)):
                for p in range(1, n):
                    sum_copy(j, p, me).wait_send()
            for p in range(1, n):
                norm_copy(p, lax.rem(me - p + n, n)).wait_recv()
                norm_copy(p, me).wait_send()
        relay(h)
        if h >= 1:
            drain(h - 1)
    drain(n - 2)


def store(n, site, kept, *refs):
    count = 9
    sources, gains = refs[:count], refs[count]
    targets, handed, sem = refs[count + 1 : 2 * count + 1], refs[2 * count + 1], refs[-1]
    me, first, last = waits(n, site)
    depth, width = sources[0].shape[0] // n, sources[0].shape[1]
    copies = []
    for k in range(1, count):
        copies.append(pltpu.make_async_copy(sources[k], targets[k], sem.at[len(copies)]))
    maybe = []
    for o in range(n):
        rows = pl.ds(o * depth, depth)
        if kept < width:
            part = (rows, pl.ds(0, width - kept))
            copies.append(
                pltpu.make_async_copy(
                    sources[0].at[part], targets[0].at[part], sem.at[len(copies)]
                )
            )
        lacks = jnp.bool_(False)
        if o == 1:
            lacks = lacks | first
        if o == n - 2:
            lacks = lacks | last
        part = (rows, pl.ds(width - kept, kept))
        maybe.append(
            (
                jnp.logical_not(lacks),
                pltpu.make_async_copy(
                    sources[0].at[part], targets[0].at[part], sem.at[count - 1 + n + o]
                ),
            )
        )
    for copy in copies:
        copy.start()
    for has, copy in maybe:
        pl.when(has)(copy.start)
    handed[...] = gains[...]
    for copy in copies:
        copy.wait()
    for has, copy in maybe:
        pl.when(has)(copy.wait)


def finish_gather(n, wide, site, final, gains, piece, serve, send, recv, norm_send, norm_recv):
    me, first, last = waits(n, site)
    late = lax.axis_index("site") == site - 1
    col = lax.axis_index("width")
    depth, kept = piece.shape
    width = final.shape[1]
    keeps = (late & (me == n - 2), late & (me == 1))
    lacks = (last, first)
    step = (1, -1)

    barrier = pltpu.get_barrier_semaphore()
    for p in range(1, wide):
        pl.semaphore_signal(
            barrier, inc=1, device_id={"width": lax.rem(col + p, wide)}, device_id_type=MESH
        )
    for d in (0, 1):
        for has, way in ((keeps[d], step[d]), (lacks[d], -step[d])):
            @pl.when(has)
            def _(way=way):
                pl.semaphore_signal(
                    barrier, inc=1, device_id={"rows": lax.rem(me + way + n, n)},
                    device_id_type=MESH,
                )
    extra = sum(x.astype(jnp.int32) for x in (*keeps, *lacks))
    pl.semaphore_wait(barrier, wide - 1 + extra)

    def tail(d):
        rows = pl.ds(pl.multiple_of(me * depth, depth), depth)
        return pltpu.make_async_remote_copy(
            src_ref=final.at[rows, pl.ds(width - kept, kept)], dst_ref=piece,
            send_sem=send.at[d], recv_sem=recv.at[d],
            device_id={"rows": lax.rem(me + step[d] + n, n)}, device_id_type=MESH,
        )

    def norm_copy(p, slot):
        return pltpu.make_async_remote_copy(
            src_ref=gains, dst_ref=serve.at[:, slot],
            send_sem=norm_send.at[p], recv_sem=norm_recv.at[p],
            device_id={"width": lax.rem(col + p, wide)}, device_id_type=MESH,
        )

    for d in (0, 1):
        pl.when(keeps[d])(tail(d).start)
    for p in range(1, wide):
        norm_copy(p, col).start()
    serve[:, col] = gains[...]
    for p in range(1, wide):
        norm_copy(p, lax.rem(col - p + wide, wide)).wait_recv()
        norm_copy(p, col).wait_send()
    for d in (0, 1):
        pl.when(keeps[d])(tail(d).wait_send)
        pl.when(lacks[d])(tail(d).wait_recv)


def finish_store(n, site, query, piece, serve, out, served, sem):
    me, first, last = waits(n, site)
    depth, kept = piece.shape
    width = out.shape[1]
    copies = [(None, pltpu.make_async_copy(serve, served, sem.at[0]))]
    for has, origin in ((first, 1), (last, n - 2)):
        part = (pl.ds(origin * depth, depth), pl.ds(width - kept, kept))
        copies.append((has, pltpu.make_async_copy(piece, out.at[part], sem.at[len(copies)])))
    for has, copy in copies:
        copy.start() if has is None else pl.when(has)(copy.start)
    for has, copy in copies:
        copy.wait() if has is None else pl.when(has)(copy.wait)


def solution(mesh):
    n, wide, site = mesh.shape["rows"], mesh.shape["width"], mesh.shape["site"]

    def per_device(*args):
        arrays, (norm_train, norm_step) = args[:9], args[9:]
        depth = arrays[0].shape[0]
        widths = [arrays[3 * a].shape[1] for a in range(3)]
        chunks = chunks_of(widths)
        count = len(chunks)
        kept = widths[0] - chunks[late_of(chunks)][1]
        part = norm_train.shape[0]
        lanes = 128 if part % 128 == 0 else part
        norms = [x.reshape(part // lanes, lanes) for x in (norm_train, norm_step)]
        vmem, dma, hbm = pltpu.VMEM, pltpu.SemaphoreType.DMA, pltpu.HBM
        in_vmem, in_hbm = pl.BlockSpec(memory_space=vmem), pl.BlockSpec(memory_space=hbm)

        def pinned(x):
            return pltpu.with_memory_space_constraint(x, vmem)

        def shaped(x):
            return jax.ShapeDtypeStruct(x.shape, x.dtype)

        out_shape = (
            [vmem((n * depth, w), jnp.bfloat16) for w in widths]
            + [vmem((1, w), jnp.float32) for w in widths]
            + [vmem((n, part // lanes, lanes), jnp.bfloat16)]
            + [vmem((depth, w), jnp.float32) for w in widths]
        )
        padded = sum(-(-w // 128) * 128 for w in widths)
        outside = padded * depth * (2 * n + 4) + (1 << 20)
        outs = pl.pallas_call(
            functools.partial(gather, n, site, chunks),
            out_shape=out_shape,
            in_specs=[in_hbm] * 11,
            out_specs=[in_vmem] * 10,
            scratch_shapes=[vmem((depth, w), jnp.float32) for w in widths for _ in range(3)]
            + [
                vmem((2, part // lanes, lanes), jnp.float32),
                vmem((count, n, 1, 128), jnp.float32),
                dma((count, 3)),
                dma((2,)),
                dma((count, n)),
                dma((count, n)),
                dma((2, n - 1, count)),
                dma((2, n - 1, count)),
                dma((n,)),
                dma((n,)),
            ],
            compiler_params=pltpu.CompilerParams(
                collective_id=0,
                has_side_effects=True,
                vmem_limit_bytes=60 * (1 << 20) - outside,
            ),
        )(*arrays, *norms)
        outs = [pinned(x) for x in outs]
        first = outs[0:6] + outs[7:10]
        stored = pl.pallas_call(
            functools.partial(store, n, site, kept),
            out_shape=[shaped(x) for x in first] + [out_shape[6]],
            in_specs=[in_vmem] * 10,
            out_specs=[in_hbm] * 9 + [in_vmem],
            scratch_shapes=[dma((8 + 2 * n,))],
            compiler_params=pltpu.CompilerParams(vmem_limit_bytes=1 << 20),
        )(*first, outs[6])
        piece, serve = pl.pallas_call(
            functools.partial(finish_gather, n, wide, site),
            out_shape=[
                vmem((depth, kept), jnp.bfloat16),
                vmem((n, wide, part // lanes, lanes), jnp.bfloat16),
            ],
            in_specs=[in_vmem] * 2,
            out_specs=[in_vmem] * 2,
            scratch_shapes=[dma((2,)), dma((2,)), dma((wide,)), dma((wide,))],
            compiler_params=pltpu.CompilerParams(
                collective_id=1, has_side_effects=True, vmem_limit_bytes=1 << 20
            ),
        )(outs[0], pinned(stored[9]))
        query, serve = pl.pallas_call(
            functools.partial(finish_store, n, site),
            out_shape=[shaped(stored[0]), shaped(serve)],
            in_specs=[in_hbm, in_vmem, in_vmem],
            out_specs=[in_hbm] * 2,
            scratch_shapes=[dma((3,))],
            input_output_aliases={0: 0},
            compiler_params=pltpu.CompilerParams(vmem_limit_bytes=1 << 20),
        )(stored[0], pinned(piece), pinned(serve))
        return (
            query,
            *stored[1:3],
            *(c.reshape(-1) for c in stored[3:6]),
            serve.reshape(-1),
            *stored[6:9],
        )

    cut = P(("site", "rows"), "width")
    return jax.shard_map(
        per_device,
        mesh=mesh,
        in_specs=(cut,) * 9 + (P(("site", "rows", "width")),) * 2,
        out_specs=(P("site", "width"),) * 3
        + (P(("site", "width")),) * 3
        + (P("site"),)
        + (cut,) * 3,
        check_vma=False,
    )
```

```python
import functools

import jax
import jax.numpy as jnp
from jax import lax
from jax.experimental import pallas as pl
from jax.experimental.pallas import tpu as pltpu
from jax.sharding import PartitionSpec as P

learn_rate = 0.02
decay_rate = 0.05
tiny_value = 1e-08

LEAD = 4
AHEAD = 4
HELD = 4, 8
MESH = pl.DeviceIdType.MESH


def chunks_of(widths):
    out = []
    for a, width in enumerate(widths):
        step = 128 if width % 128 == 0 else width
        out += [(a, c, step) for c in range(0, width, step)]
    return out


def late_of(chunks):
    count = sum(1 for ch in chunks if ch[0] == 0)
    return count - max(1, count * HELD[0] // HELD[1])


def waits(n, site):
    me = lax.axis_index("rows")
    late = lax.axis_index("site") == site - 1
    return me, late & (me == 0), late & (me == n - 1)


def gather(n, wide, site, chunks, *refs):
    inputs, norms = [refs[0:3], refs[3:6], refs[6:9]], refs[9:11]
    finals, columns, serve, results = refs[11:14], refs[14:17], refs[17], refs[18:21]
    held = [refs[21:24], refs[24:27], refs[27:30]]
    gain, sums, in_sem, gain_sem, sum_send, sum_recv, send, recv = refs[30:38]
    norm_send, norm_recv, wide_send, wide_recv = refs[38:]
    me, first, last = waits(n, site)
    late = lax.axis_index("site") == site - 1
    col = lax.axis_index("width")
    depth = results[0].shape[0]
    block = min(depth, 64)
    split = late_of(chunks)
    counts = [sum(1 for ch in chunks if ch[0] == a) for a in range(3)]
    bases = [sum(counts[:a]) for a in range(3)]

    barrier = pltpu.get_barrier_semaphore()

    def load(j, k):
        a, c, cw = chunks[j]
        return pltpu.make_async_copy(
            inputs[a][k].at[:, pl.ds(c, cw)], held[a][k].at[:, pl.ds(c, cw)], in_sem.at[j, k]
        )

    for p in range(1, n):
        pl.semaphore_signal(
            barrier, inc=1, device_id={"rows": lax.rem(me + p, n)}, device_id_type=MESH
        )
    for p in range(1, wide):
        pl.semaphore_signal(
            barrier, inc=1, device_id={"width": lax.rem(col + p, wide)}, device_id_type=MESH
        )
    ahead = min(AHEAD, len(chunks))
    for j in range(ahead):
        for k in range(3):
            load(j, k).start()
    for k in range(2):
        pltpu.make_async_copy(norms[k], gain.at[k], gain_sem.at[k]).start()

    def update(j):
        a, c, cw = chunks[j]
        for k in range(3):
            load(j, k).wait()
        if j + ahead < len(chunks):
            for k in range(3):
                load(j + ahead, k).start()
        weight, moment, square = held[a]
        cols = pl.ds(c, cw)

        def body(i, acc):
            rows = pl.ds(pl.multiple_of(i * block, block), block)
            w = weight[rows, cols]
            r = w - learn_rate * (
                moment[rows, cols] / (jnp.sqrt(square[rows, cols]) + tiny_value) + decay_rate * w
            )
            results[a][rows, cols] = r
            return acc + jnp.sum((r * r).reshape(block // 8, 8, cw), axis=0)

        acc = lax.fori_loop(0, depth // block, body, jnp.zeros((8, cw), jnp.float32))
        sums[j, me, :, pl.ds(0, cw)] = jnp.sum(acc, axis=0, keepdims=True)

    def sum_copy(j, p, slot):
        return pltpu.make_async_remote_copy(
            src_ref=sums.at[j, me], dst_ref=sums.at[j, slot],
            send_sem=sum_send.at[j, p], recv_sem=sum_recv.at[j, p],
            device_id={"rows": lax.rem(me + p, n)}, device_id_type=MESH,
        )

    def norm_copy(p, slot):
        return pltpu.make_async_remote_copy(
            src_ref=serve.at[me, col], dst_ref=serve.at[slot, col],
            send_sem=norm_send.at[p], recv_sem=norm_recv.at[p],
            device_id={"rows": lax.rem(me + p, n)}, device_id_type=MESH,
        )

    def wide_copy(p, slot):
        return pltpu.make_async_remote_copy(
            src_ref=serve.at[:, col], dst_ref=serve.at[:, slot],
            send_sem=wide_send.at[p], recv_sem=wide_recv.at[p],
            device_id={"width": lax.rem(col + p, wide)}, device_id_type=MESH,
        )

    has_next = (me < n - 1, me > 0)
    step = (1, -1)
    keeps = (late & (me == n - 2), late & (me == 1))
    lacks = (last, first)

    def pass_on(d, h, j, a, cols, origin):
        rows = pl.ds(pl.multiple_of(origin * depth, depth), depth)
        return pltpu.make_async_remote_copy(
            src_ref=finals[a].at[rows, cols], dst_ref=finals[a].at[rows, cols],
            send_sem=send.at[d, h, j], recv_sem=recv.at[d, h, j],
            device_id={"rows": lax.rem(me + step[d] + n, n)}, device_id_type=MESH,
        )

    def finish(j):
        a, c, cw = chunks[j]
        cols = pl.ds(c, cw)
        for p in range(1, n):
            sum_copy(j, p, lax.rem(me - p + n, n)).wait_recv()
        total = sums[j, 0, :, pl.ds(0, cw)]
        for p in range(1, n):
            total = total + sums[j, p, :, pl.ds(0, cw)]
        scale = jnp.sqrt(total)
        columns[a][:, cols] = scale
        inverse = 1.0 / scale

        def body(i, carry):
            rows = pl.ds(pl.multiple_of(i * block, block), block)
            mine = pl.ds(pl.multiple_of(me * depth + i * block, block), block)
            finals[a][mine, cols] = (results[a][rows, cols] * inverse).astype(jnp.bfloat16)
            return carry

        lax.fori_loop(0, depth // block, body, 0)
        for d in (0, 1):
            goes = has_next[d]
            if a == 0 and j >= split:
                goes = goes & jnp.logical_not(keeps[d])

            @pl.when(goes)
            def _(d=d):
                pass_on(d, 0, j, a, cols, me).start()

    ready = 0
    for j in range(len(chunks)):
        while ready < min(len(chunks), LEAD * (j + 1)):
            update(ready)
            if ready == 0:
                pl.semaphore_wait(barrier, n + wide - 2)
            for p in range(1, n):
                sum_copy(ready, p, me).start()
            ready += 1
        finish(j)

    for k in range(2):
        pltpu.make_async_copy(norms[k], gain.at[k], gain_sem.at[k]).wait()
    serve[me, col] = (gain[0] + gain[1]).astype(jnp.bfloat16)
    for p in range(1, n):
        norm_copy(p, me).start()

    def span(a, cut, visit):
        cw = chunks[bases[a]][2]

        def body(k, carry):
            start = pl.multiple_of(k * cw, 128) if counts[a] > 1 else 0
            visit(bases[a] + k, a, pl.ds(start, cw))
            return carry

        low, high = cut
        if counts[a] > 1:
            lax.fori_loop(low, high, body, 0)
        elif high > low:
            body(0, 0)

    def parts(a, h):
        if a == 0 and h == 0:
            return ((0, split), False), ((split, counts[0]), True)
        return (((0, counts[a]), False),)

    def relay(h):
        for a in range(3):
            for cut, tail in parts(a, h):

                def visit(j, a, cols, tail=tail):
                    for d in (0, 1):
                        origin = me - step[d] * (h + 1)
                        comes = (origin >= 0) & (origin < n)
                        if tail:
                            comes = comes & jnp.logical_not(lacks[d])

                        @pl.when(comes)
                        def _(d=d, origin=origin):
                            pass_on(d, h, j, a, cols, origin).wait_recv()

                            if h + 1 < n - 1:
                                @pl.when(has_next[d])
                                def _():
                                    pass_on(d, h + 1, j, a, cols, origin).start()

                span(a, cut, visit)

    def drain(h):
        for d in (0, 1):
            origin = me - step[d] * h
            for a in range(3):
                for cut, tail in parts(a, h):
                    went = has_next[d] & (origin >= 0) & (origin < n)
                    if tail:
                        went = went & jnp.logical_not(keeps[d])

                    @pl.when(went)
                    def _(d=d, a=a, cut=cut, origin=origin):
                        span(
                            a, cut,
                            lambda j, a, cols: pass_on(d, h, j, a, cols, origin).wait_send(),
                        )

    for h in range(n - 1):
        if h == n - 2:
            for j in range(len(chunks)):
                for p in range(1, n):
                    sum_copy(j, p, me).wait_send()
            for p in range(1, n):
                norm_copy(p, me).wait_send()
            for p in range(1, wide):
                wide_copy(p, col).wait_send()
                wide_copy(p, lax.rem(col - p + wide, wide)).wait_recv()
        relay(h)
        if h == 0:
            for p in range(1, n):
                norm_copy(p, lax.rem(me - p + n, n)).wait_recv()
            for p in range(1, wide):
                wide_copy(p, col).start()
        if h >= 1:
            drain(h - 1)
    drain(n - 2)


def store(n, site, kept, *refs):
    count = 10
    sources, targets = refs[:count], refs[count : 2 * count]
    handed, sem = refs[2 * count :]
    me, first, last = waits(n, site)
    depth, width = sources[0].shape[0] // n, sources[0].shape[1]
    copies = []
    for k in range(1, count):
        copies.append(pltpu.make_async_copy(sources[k], targets[k], sem.at[len(copies)]))
    maybe = []
    for o in range(n):
        rows = pl.ds(o * depth, depth)
        if kept < width:
            part = (rows, pl.ds(0, width - kept))
            copies.append(
                pltpu.make_async_copy(
                    sources[0].at[part], targets[0].at[part], sem.at[len(copies)]
                )
            )
        lacks = jnp.bool_(False)
        if o == 1:
            lacks = lacks | first
        if o == n - 2:
            lacks = lacks | last
        part = (rows, pl.ds(width - kept, kept))
        maybe.append(
            (
                jnp.logical_not(lacks),
                pltpu.make_async_copy(
                    sources[0].at[part], targets[0].at[part], sem.at[count - 1 + n + o]
                ),
            )
        )
    for copy in copies:
        copy.start()
    for has, copy in maybe:
        pl.when(has)(copy.start)
    handed[...] = sources[3][...]
    for copy in copies:
        copy.wait()
    for has, copy in maybe:
        pl.when(has)(copy.wait)


def finish_gather(n, site, final, after, piece, send, recv):
    me, first, last = waits(n, site)
    late = lax.axis_index("site") == site - 1
    depth, kept = piece.shape
    width = final.shape[1]
    keeps = (late & (me == n - 2), late & (me == 1))
    lacks = (last, first)
    step = (1, -1)

    barrier = pltpu.get_barrier_semaphore()
    count = jnp.int32(0)
    for d in (0, 1):
        for has, way in ((keeps[d], step[d]), (lacks[d], -step[d])):
            count = count + has.astype(jnp.int32)

            @pl.when(has)
            def _(way=way):
                pl.semaphore_signal(
                    barrier, inc=1, device_id={"rows": lax.rem(me + way + n, n)},
                    device_id_type=MESH,
                )

    @pl.when(count > 0)
    def _():
        pl.semaphore_wait(barrier, count)

    def tail(d):
        rows = pl.ds(pl.multiple_of(me * depth, depth), depth)
        return pltpu.make_async_remote_copy(
            src_ref=final.at[rows, pl.ds(width - kept, kept)], dst_ref=piece,
            send_sem=send.at[d], recv_sem=recv.at[d],
            device_id={"rows": lax.rem(me + step[d] + n, n)}, device_id_type=MESH,
        )

    for d in (0, 1):
        pl.when(keeps[d])(tail(d).start)
    for d in (0, 1):
        pl.when(keeps[d])(tail(d).wait_send)
        pl.when(lacks[d])(tail(d).wait_recv)


def finish_store(n, site, query, piece, out, sem):
    me, first, last = waits(n, site)
    depth, kept = piece.shape
    width = out.shape[1]
    for has, origin in ((first, 1), (last, n - 2)):
        part = (pl.ds(origin * depth, depth), pl.ds(width - kept, kept))

        @pl.when(has)
        def _(part=part):
            copy = pltpu.make_async_copy(piece, out.at[part], sem)
            copy.start()
            copy.wait()


def solution(mesh):
    n, wide, site = mesh.shape["rows"], mesh.shape["width"], mesh.shape["site"]

    def per_device(*args):
        arrays, (norm_train, norm_step) = args[:9], args[9:]
        depth = arrays[0].shape[0]
        widths = [arrays[3 * a].shape[1] for a in range(3)]
        chunks = chunks_of(widths)
        count = len(chunks)
        kept = widths[0] - chunks[late_of(chunks)][1]
        part = norm_train.shape[0]
        lanes = 128 if part % 128 == 0 else part
        norms = [x.reshape(part // lanes, lanes) for x in (norm_train, norm_step)]
        vmem, dma, hbm = pltpu.VMEM, pltpu.SemaphoreType.DMA, pltpu.HBM
        in_vmem, in_hbm = pl.BlockSpec(memory_space=vmem), pl.BlockSpec(memory_space=hbm)

        def pinned(x):
            return pltpu.with_memory_space_constraint(x, vmem)

        def shaped(x):
            return jax.ShapeDtypeStruct(x.shape, x.dtype)

        out_shape = (
            [vmem((n * depth, w), jnp.bfloat16) for w in widths]
            + [vmem((1, w), jnp.float32) for w in widths]
            + [vmem((n, wide, part // lanes, lanes), jnp.bfloat16)]
            + [vmem((depth, w), jnp.float32) for w in widths]
        )
        padded = sum(-(-w // 128) * 128 for w in widths)
        outside = padded * depth * (2 * n + 4) + (1 << 20)
        outs = pl.pallas_call(
            functools.partial(gather, n, wide, site, chunks),
            out_shape=out_shape,
            in_specs=[in_hbm] * 11,
            out_specs=[in_vmem] * 10,
            scratch_shapes=[vmem((depth, w), jnp.float32) for w in widths for _ in range(3)]
            + [
                vmem((2, part // lanes, lanes), jnp.float32),
                vmem((count, n, 1, 128), jnp.float32),
                dma((count, 3)),
                dma((2,)),
                dma((count, n)),
                dma((count, n)),
                dma((2, n - 1, count)),
                dma((2, n - 1, count)),
                dma((n,)),
                dma((n,)),
                dma((wide,)),
                dma((wide,)),
            ],
            compiler_params=pltpu.CompilerParams(
                collective_id=0,
                has_side_effects=True,
                vmem_limit_bytes=60 * (1 << 20) - outside,
            ),
        )(*arrays, *norms)
        outs = [pinned(x) for x in outs]
        stored = pl.pallas_call(
            functools.partial(store, n, site, kept),
            out_shape=[shaped(x) for x in outs] + [out_shape[3]],
            in_specs=[in_vmem] * 10,
            out_specs=[in_hbm] * 10 + [in_vmem],
            scratch_shapes=[dma((9 + 2 * n,))],
            compiler_params=pltpu.CompilerParams(vmem_limit_bytes=1 << 20),
        )(*outs)
        piece = pl.pallas_call(
            functools.partial(finish_gather, n, site),
            out_shape=vmem((depth, kept), jnp.bfloat16),
            in_specs=[in_vmem] * 2,
            out_specs=in_vmem,
            scratch_shapes=[dma((2,)), dma((2,))],
            compiler_params=pltpu.CompilerParams(
                collective_id=1, has_side_effects=True, vmem_limit_bytes=1 << 20
            ),
        )(outs[0], pinned(stored[10]))
        query = pl.pallas_call(
            functools.partial(finish_store, n, site),
            out_shape=shaped(stored[0]),
            in_specs=[in_hbm, in_vmem],
            out_specs=in_hbm,
            scratch_shapes=[pltpu.SemaphoreType.DMA],
            input_output_aliases={0: 0},
            compiler_params=pltpu.CompilerParams(vmem_limit_bytes=1 << 20),
        )(stored[0], pinned(piece))
        return (
            query,
            *stored[1:3],
            *(c.reshape(-1) for c in stored[3:6]),
            stored[6].reshape(-1),
            *stored[7:10],
        )

    cut = P(("site", "rows"), "width")
    return jax.shard_map(
        per_device,
        mesh=mesh,
        in_specs=(cut,) * 9 + (P(("site", "rows", "width")),) * 2,
        out_specs=(P("site", "width"),) * 3
        + (P(("site", "width")),) * 3
        + (P("site"),)
        + (cut,) * 3,
        check_vma=False,
    )
```

```python
import functools

import jax
import jax.numpy as jnp
from jax import lax
from jax.experimental import pallas as pl
from jax.experimental.pallas import tpu as pltpu
from jax.sharding import PartitionSpec as P

learn_rate = 0.02
decay_rate = 0.05
tiny_value = 1e-08

LEAD = 4
AHEAD = 4
HELD = 4, 8
HEAD = 5, 16
MESH = pl.DeviceIdType.MESH


def chunks_of(widths):
    out = []
    for a, width in enumerate(widths):
        step = 128 if width % 128 == 0 else width
        out += [(a, c, step) for c in range(0, width, step)]
    return out


def late_of(chunks):
    count = sum(1 for ch in chunks if ch[0] == 0)
    return count - max(1, count * HELD[0] // HELD[1])


def head_of(depth, block):
    return block * max(1, depth // block * HEAD[0] // HEAD[1])


def block_of(depth):
    return min(depth, 64)


def waits(n, site):
    me = lax.axis_index("rows")
    late = lax.axis_index("site") == site - 1
    return me, late & (me == 0), late & (me == n - 1)


def gather(n, wide, site, chunks, *refs):
    inputs, norms = [refs[0:3], refs[3:6], refs[6:9]], refs[9:11]
    finals, columns, serve, results = refs[11:14], refs[14:17], refs[17], refs[18:21]
    held = [refs[21:24], refs[24:27], refs[27:30]]
    gain, sums, in_sem, gain_sem, sum_send, sum_recv, send, recv = refs[30:38]
    norm_send, norm_recv, wide_send, wide_recv, raw, top_sem, raw_send, raw_recv = refs[38:]
    me, first, last = waits(n, site)
    late = lax.axis_index("site") == site - 1
    col = lax.axis_index("width")
    depth = results[0].shape[0]
    block = block_of(depth)
    top = head_of(depth, block)
    split = late_of(chunks)
    counts = [sum(1 for ch in chunks if ch[0] == a) for a in range(3)]
    bases = [sum(counts[:a]) for a in range(3)]

    barrier = pltpu.get_barrier_semaphore()

    def load(j, k):
        a, c, cw = chunks[j]
        part = (pl.ds(0, depth) if j else pl.ds(top, depth - top), pl.ds(c, cw))
        return pltpu.make_async_copy(
            inputs[a][k].at[part], held[a][k].at[part], in_sem.at[j, k]
        )

    def load_top(k):
        part = (pl.ds(0, top), pl.ds(0, chunks[0][2]))
        return pltpu.make_async_copy(inputs[0][k].at[part], held[0][k].at[part], top_sem.at[k])

    for p in range(1, n):
        pl.semaphore_signal(
            barrier, inc=1, device_id={"rows": lax.rem(me + p, n)}, device_id_type=MESH
        )
    for p in range(1, wide):
        pl.semaphore_signal(
            barrier, inc=1, device_id={"width": lax.rem(col + p, wide)}, device_id_type=MESH
        )
    ahead = min(AHEAD, len(chunks))
    for k in range(3):
        load_top(k).start()
    for j in range(ahead):
        for k in range(3):
            load(j, k).start()
    for k in range(2):
        pltpu.make_async_copy(norms[k], gain.at[k], gain_sem.at[k]).start()

    def rows_of(j, low, high, acc):
        a, c, cw = chunks[j]
        weight, moment, square = held[a]
        cols = pl.ds(c, cw)

        def body(i, acc):
            rows = pl.ds(pl.multiple_of(i * block, block), block)
            w = weight[rows, cols]
            r = w - learn_rate * (
                moment[rows, cols] / (jnp.sqrt(square[rows, cols]) + tiny_value) + decay_rate * w
            )
            results[a][rows, cols] = r
            return acc + jnp.sum((r * r).reshape(block // 8, 8, cw), axis=0)

        return lax.fori_loop(low // block, high // block, body, acc)

    def update(j, low, acc):
        cw = chunks[j][2]
        for k in range(3):
            load(j, k).wait()
        if j + ahead < len(chunks):
            for k in range(3):
                load(j + ahead, k).start()
        acc = rows_of(j, low, depth, acc)
        sums[j, me, :, pl.ds(0, cw)] = jnp.sum(acc, axis=0, keepdims=True)

    def sum_copy(j, p, slot):
        return pltpu.make_async_remote_copy(
            src_ref=sums.at[j, me], dst_ref=sums.at[j, slot],
            send_sem=sum_send.at[j, p], recv_sem=sum_recv.at[j, p],
            device_id={"rows": lax.rem(me + p, n)}, device_id_type=MESH,
        )

    def norm_copy(p, slot):
        return pltpu.make_async_remote_copy(
            src_ref=serve.at[me, col], dst_ref=serve.at[slot, col],
            send_sem=norm_send.at[p], recv_sem=norm_recv.at[p],
            device_id={"rows": lax.rem(me + p, n)}, device_id_type=MESH,
        )

    def wide_copy(p, slot):
        return pltpu.make_async_remote_copy(
            src_ref=serve.at[:, col], dst_ref=serve.at[:, slot],
            send_sem=wide_send.at[p], recv_sem=wide_recv.at[p],
            device_id={"width": lax.rem(col + p, wide)}, device_id_type=MESH,
        )

    has_next = (me < n - 1, me > 0)
    step = (1, -1)
    keeps = (late & (me == n - 2), late & (me == 1))
    lacks = (last, first)

    opens = ((me == n - 2), (me == 1))
    opened = ((me == n - 1), (me == 0))

    def raw_copy(d):
        return pltpu.make_async_remote_copy(
            src_ref=results[0].at[pl.ds(0, top), pl.ds(0, chunks[0][2])], dst_ref=raw,
            send_sem=raw_send.at[d], recv_sem=raw_recv.at[d],
            device_id={"rows": lax.rem(me + step[d] + n, n)}, device_id_type=MESH,
        )

    def pass_on(d, h, j, a, cols, origin, skip=0):
        rows = pl.ds(pl.multiple_of(origin * depth + skip, block), depth - skip)
        return pltpu.make_async_remote_copy(
            src_ref=finals[a].at[rows, cols], dst_ref=finals[a].at[rows, cols],
            send_sem=send.at[d, h, j], recv_sem=recv.at[d, h, j],
            device_id={"rows": lax.rem(me + step[d] + n, n)}, device_id_type=MESH,
        )

    def finish(j):
        a, c, cw = chunks[j]
        cols = pl.ds(c, cw)
        for p in range(1, n):
            sum_copy(j, p, lax.rem(me - p + n, n)).wait_recv()
        total = sums[j, 0, :, pl.ds(0, cw)]
        for p in range(1, n):
            total = total + sums[j, p, :, pl.ds(0, cw)]
        scale = jnp.sqrt(total)
        columns[a][:, cols] = scale
        inverse = 1.0 / scale

        def body(i, carry):
            rows = pl.ds(pl.multiple_of(i * block, block), block)
            mine = pl.ds(pl.multiple_of(me * depth + i * block, block), block)
            finals[a][mine, cols] = (results[a][rows, cols] * inverse).astype(jnp.bfloat16)
            return carry

        lax.fori_loop(0, depth // block, body, 0)
        for d in (0, 1):
            goes = has_next[d]
            if a == 0 and j >= split:
                goes = goes & jnp.logical_not(keeps[d])
            if j == 0:
                goes = goes & jnp.logical_not(opens[d])
                pl.when(opens[d])(pass_on(d, 0, j, a, cols, me, top).start)

            @pl.when(goes)
            def _(d=d):
                pass_on(d, 0, j, a, cols, me).start()

    ready = 0
    for j in range(len(chunks)):
        while ready < min(len(chunks), LEAD * (j + 1)):
            acc, low = jnp.zeros((8, chunks[ready][2]), jnp.float32), 0
            if ready == 0:
                low = top
                for k in range(3):
                    load_top(k).wait()
                acc = rows_of(0, 0, top, acc)
                pl.semaphore_wait(barrier, n + wide - 2)
                for d in (0, 1):
                    pl.when(opens[d])(raw_copy(d).start)
            update(ready, low, acc)
            for p in range(1, n):
                sum_copy(ready, p, me).start()
            ready += 1
        finish(j)

    for k in range(2):
        pltpu.make_async_copy(norms[k], gain.at[k], gain_sem.at[k]).wait()
    serve[me, col] = (gain[0] + gain[1]).astype(jnp.bfloat16)
    for p in range(1, n):
        norm_copy(p, me).start()

    for d in (0, 1):
        @pl.when(opened[d])
        def _(d=d):
            raw_copy(d).wait_recv()
            cw = chunks[0][2]
            inverse = 1.0 / columns[0][:, pl.ds(0, cw)]
            origin = (n - 2, 1)[d] * depth

            def body(i, carry):
                rows = pl.ds(pl.multiple_of(i * block, block), block)
                theirs = pl.ds(pl.multiple_of(origin + i * block, block), block)
                finals[0][theirs, pl.ds(0, cw)] = (raw[rows, :] * inverse).astype(jnp.bfloat16)
                return carry

            lax.fori_loop(0, top // block, body, 0)

    def span(a, cut, visit):
        cw = chunks[bases[a]][2]

        def body(k, carry):
            start = pl.multiple_of(k * cw, 128) if counts[a] > 1 else 0
            visit(bases[a] + k, a, pl.ds(start, cw))
            return carry

        low, high = cut
        if counts[a] > 1:
            lax.fori_loop(low, high, body, 0)
        elif high > low:
            body(0, 0)

    whole, tail, head = range(3)

    def parts(a, h):
        if a == 0 and h == 0:
            return ((0, 1), head), ((1, split), whole), ((split, counts[0]), tail)
        return (((0, counts[a]), whole),)

    def relay(h):
        for a in range(3):
            for cut, kind in parts(a, h):

                def visit(j, a, cols, kind=kind):
                    for d in (0, 1):
                        origin = me - step[d] * (h + 1)
                        comes = (origin >= 0) & (origin < n)
                        if kind == tail:
                            comes = comes & jnp.logical_not(lacks[d])
                        if kind == head:
                            comes = comes & jnp.logical_not(opened[d])
                            pl.when(opened[d])(
                                pass_on(d, h, j, a, cols, origin, top).wait_recv
                            )

                        @pl.when(comes)
                        def _(d=d, origin=origin):
                            pass_on(d, h, j, a, cols, origin).wait_recv()

                            if h + 1 < n - 1:
                                @pl.when(has_next[d])
                                def _():
                                    pass_on(d, h + 1, j, a, cols, origin).start()

                span(a, cut, visit)

    def drain(h):
        for d in (0, 1):
            origin = me - step[d] * h
            for a in range(3):
                for cut, kind in parts(a, h):
                    went = has_next[d] & (origin >= 0) & (origin < n)
                    if kind == tail:
                        went = went & jnp.logical_not(keeps[d])
                    if kind == head:
                        went = went & jnp.logical_not(opens[d])

                        @pl.when(opens[d])
                        def _(d=d):
                            raw_copy(d).wait_send()
                            cols = pl.ds(0, chunks[0][2])
                            pass_on(d, 0, 0, 0, cols, me, top).wait_send()

                    @pl.when(went)
                    def _(d=d, a=a, cut=cut, origin=origin):
                        span(
                            a, cut,
                            lambda j, a, cols: pass_on(d, h, j, a, cols, origin).wait_send(),
                        )

    for h in range(n - 1):
        if h == n - 2:
            for j in range(len(chunks)):
                for p in range(1, n):
                    sum_copy(j, p, me).wait_send()
            for p in range(1, n):
                norm_copy(p, me).wait_send()
            for p in range(1, wide):
                wide_copy(p, col).wait_send()
                wide_copy(p, lax.rem(col - p + wide, wide)).wait_recv()
        relay(h)
        if h == 0:
            for p in range(1, n):
                norm_copy(p, lax.rem(me - p + n, n)).wait_recv()
            for p in range(1, wide):
                wide_copy(p, col).start()
        if h >= 1:
            drain(h - 1)
    drain(n - 2)


def store(n, site, kept, *refs):
    count = 10
    sources, targets = refs[:count], refs[count : 2 * count]
    handed, sem = refs[2 * count :]
    me, first, last = waits(n, site)
    depth, width = sources[0].shape[0] // n, sources[0].shape[1]
    copies = []
    for k in range(1, count):
        copies.append(pltpu.make_async_copy(sources[k], targets[k], sem.at[len(copies)]))
    maybe = []
    for o in range(n):
        rows = pl.ds(o * depth, depth)
        if kept < width:
            part = (rows, pl.ds(0, width - kept))
            copies.append(
                pltpu.make_async_copy(
                    sources[0].at[part], targets[0].at[part], sem.at[len(copies)]
                )
            )
        lacks = jnp.bool_(False)
        if o == 1:
            lacks = lacks | first
        if o == n - 2:
            lacks = lacks | last
        part = (rows, pl.ds(width - kept, kept))
        maybe.append(
            (
                jnp.logical_not(lacks),
                pltpu.make_async_copy(
                    sources[0].at[part], targets[0].at[part], sem.at[count - 1 + n + o]
                ),
            )
        )
    for copy in copies:
        copy.start()
    for has, copy in maybe:
        pl.when(has)(copy.start)
    handed[...] = sources[3][...]
    for copy in copies:
        copy.wait()
    for has, copy in maybe:
        pl.when(has)(copy.wait)


def finish_gather(n, site, final, after, piece, send, recv):
    me, first, last = waits(n, site)
    late = lax.axis_index("site") == site - 1
    depth, kept = piece.shape
    width = final.shape[1]
    keeps = (late & (me == n - 2), late & (me == 1))
    lacks = (last, first)
    step = (1, -1)

    barrier = pltpu.get_barrier_semaphore()
    count = jnp.int32(0)
    for d in (0, 1):
        for has, way in ((keeps[d], step[d]), (lacks[d], -step[d])):
            count = count + has.astype(jnp.int32)

            @pl.when(has)
            def _(way=way):
                pl.semaphore_signal(
                    barrier, inc=1, device_id={"rows": lax.rem(me + way + n, n)},
                    device_id_type=MESH,
                )

    @pl.when(count > 0)
    def _():
        pl.semaphore_wait(barrier, count)

    def tail(d):
        rows = pl.ds(pl.multiple_of(me * depth, depth), depth)
        return pltpu.make_async_remote_copy(
            src_ref=final.at[rows, pl.ds(width - kept, kept)], dst_ref=piece,
            send_sem=send.at[d], recv_sem=recv.at[d],
            device_id={"rows": lax.rem(me + step[d] + n, n)}, device_id_type=MESH,
        )

    for d in (0, 1):
        pl.when(keeps[d])(tail(d).start)
    for d in (0, 1):
        pl.when(keeps[d])(tail(d).wait_send)
        pl.when(lacks[d])(tail(d).wait_recv)


def finish_store(n, site, query, piece, out, sem):
    me, first, last = waits(n, site)
    depth, kept = piece.shape
    width = out.shape[1]
    for has, origin in ((first, 1), (last, n - 2)):
        part = (pl.ds(origin * depth, depth), pl.ds(width - kept, kept))

        @pl.when(has)
        def _(part=part):
            copy = pltpu.make_async_copy(piece, out.at[part], sem)
            copy.start()
            copy.wait()


def solution(mesh):
    n, wide, site = mesh.shape["rows"], mesh.shape["width"], mesh.shape["site"]

    def per_device(*args):
        arrays, (norm_train, norm_step) = args[:9], args[9:]
        depth = arrays[0].shape[0]
        widths = [arrays[3 * a].shape[1] for a in range(3)]
        chunks = chunks_of(widths)
        count = len(chunks)
        kept = widths[0] - chunks[late_of(chunks)][1]
        part = norm_train.shape[0]
        lanes = 128 if part % 128 == 0 else part
        norms = [x.reshape(part // lanes, lanes) for x in (norm_train, norm_step)]
        vmem, dma, hbm = pltpu.VMEM, pltpu.SemaphoreType.DMA, pltpu.HBM
        in_vmem, in_hbm = pl.BlockSpec(memory_space=vmem), pl.BlockSpec(memory_space=hbm)

        def pinned(x):
            return pltpu.with_memory_space_constraint(x, vmem)

        def shaped(x):
            return jax.ShapeDtypeStruct(x.shape, x.dtype)

        out_shape = (
            [vmem((n * depth, w), jnp.bfloat16) for w in widths]
            + [vmem((1, w), jnp.float32) for w in widths]
            + [vmem((n, wide, part // lanes, lanes), jnp.bfloat16)]
            + [vmem((depth, w), jnp.float32) for w in widths]
        )
        padded = sum(-(-w // 128) * 128 for w in widths)
        outside = padded * depth * (2 * n + 4) + (1 << 20)
        outs = pl.pallas_call(
            functools.partial(gather, n, wide, site, chunks),
            out_shape=out_shape,
            in_specs=[in_hbm] * 11,
            out_specs=[in_vmem] * 10,
            scratch_shapes=[vmem((depth, w), jnp.float32) for w in widths for _ in range(3)]
            + [
                vmem((2, part // lanes, lanes), jnp.float32),
                vmem((count, n, 1, 128), jnp.float32),
                dma((count, 3)),
                dma((2,)),
                dma((count, n)),
                dma((count, n)),
                dma((2, n - 1, count)),
                dma((2, n - 1, count)),
                dma((n,)),
                dma((n,)),
                dma((wide,)),
                dma((wide,)),
                vmem((head_of(depth, block_of(depth)), chunks[0][2]), jnp.float32),
                dma((3,)),
                dma((2,)),
                dma((2,)),
            ],
            compiler_params=pltpu.CompilerParams(
                collective_id=0,
                has_side_effects=True,
                vmem_limit_bytes=60 * (1 << 20) - outside,
            ),
        )(*arrays, *norms)
        outs = [pinned(x) for x in outs]
        stored = pl.pallas_call(
            functools.partial(store, n, site, kept),
            out_shape=[shaped(x) for x in outs] + [out_shape[3]],
            in_specs=[in_vmem] * 10,
            out_specs=[in_hbm] * 10 + [in_vmem],
            scratch_shapes=[dma((9 + 2 * n,))],
            compiler_params=pltpu.CompilerParams(vmem_limit_bytes=1 << 20),
        )(*outs)
        piece = pl.pallas_call(
            functools.partial(finish_gather, n, site),
            out_shape=vmem((depth, kept), jnp.bfloat16),
            in_specs=[in_vmem] * 2,
            out_specs=in_vmem,
            scratch_shapes=[dma((2,)), dma((2,))],
            compiler_params=pltpu.CompilerParams(
                collective_id=1, has_side_effects=True, vmem_limit_bytes=1 << 20
            ),
        )(outs[0], pinned(stored[10]))
        query = pl.pallas_call(
            functools.partial(finish_store, n, site),
            out_shape=shaped(stored[0]),
            in_specs=[in_hbm, in_vmem],
            out_specs=in_hbm,
            scratch_shapes=[pltpu.SemaphoreType.DMA],
            input_output_aliases={0: 0},
            compiler_params=pltpu.CompilerParams(vmem_limit_bytes=1 << 20),
        )(stored[0], pinned(piece))
        return (
            query,
            *stored[1:3],
            *(c.reshape(-1) for c in stored[3:6]),
            stored[6].reshape(-1),
            *stored[7:10],
        )

    cut = P(("site", "rows"), "width")
    return jax.shard_map(
        per_device,
        mesh=mesh,
        in_specs=(cut,) * 9 + (P(("site", "rows", "width")),) * 2,
        out_specs=(P("site", "width"),) * 3
        + (P(("site", "width")),) * 3
        + (P("site"),)
        + (cut,) * 3,
        check_vma=False,
    )
```

```python
import functools

import jax
import jax.numpy as jnp
from jax import lax
from jax.experimental import pallas as pl
from jax.experimental.pallas import tpu as pltpu
from jax.sharding import PartitionSpec as P

learn_rate = 0.02
decay_rate = 0.05
tiny_value = 1e-08

LEAD = 4
AHEAD = 4
HELD = 4, 8
HEAD = 5, 16
NEAR = 3
MESH = pl.DeviceIdType.MESH


def chunks_of(widths):
    out = []
    for a, width in enumerate(widths):
        step = 128 if width % 128 == 0 else width
        out += [(a, c, step) for c in range(0, width, step)]
    return out


def late_of(chunks):
    count = sum(1 for ch in chunks if ch[0] == 0)
    return count - max(1, count * HELD[0] // HELD[1])


def head_of(depth, block):
    return block * max(1, depth // block * HEAD[0] // HEAD[1])


def block_of(depth):
    return min(depth, 64)


def waits(n, site):
    me = lax.axis_index("rows")
    late = lax.axis_index("site") == site - 1
    return me, late & (me == 0), late & (me == n - 1)


def gather(n, wide, site, chunks, *refs):
    inputs, norms = [refs[0:3], refs[3:6], refs[6:9]], refs[9:11]
    finals, columns, serve, results = refs[11:14], refs[14:17], refs[17], refs[18:21]
    held = [refs[21:24], refs[24:27], refs[27:30]]
    gain, sums, in_sem, gain_sem, sum_send, sum_recv, send, recv = refs[30:38]
    norm_send, norm_recv, wide_send, wide_recv, raw, top_sem, raw_send, raw_recv = refs[38:46]
    own, serve_send, serve_recv = refs[46:]
    me, first, last = waits(n, site)
    late = lax.axis_index("site") == site - 1
    col = lax.axis_index("width")
    depth = results[0].shape[0]
    block = block_of(depth)
    top = head_of(depth, block)
    split = late_of(chunks)
    counts = [sum(1 for ch in chunks if ch[0] == a) for a in range(3)]
    bases = [sum(counts[:a]) for a in range(3)]

    barrier = pltpu.get_barrier_semaphore()

    def load(j, k):
        a, c, cw = chunks[j]
        part = (pl.ds(0, depth) if j else pl.ds(top, depth - top), pl.ds(c, cw))
        return pltpu.make_async_copy(
            inputs[a][k].at[part], held[a][k].at[part], in_sem.at[j, k]
        )

    def load_top(k):
        part = (pl.ds(0, top), pl.ds(0, chunks[0][2]))
        return pltpu.make_async_copy(inputs[0][k].at[part], held[0][k].at[part], top_sem.at[k])

    near = [
        jnp.logical_not((me < 2) & (lax.rem(me + p, n) >= NEAR)) for p in range(1, n)
    ]
    for p in range(1, n):
        @pl.when(jnp.logical_not((me >= NEAR) & (lax.rem(me + p, n) < 2)))
        def _(p=p):
            pl.semaphore_signal(
                barrier, inc=1, device_id={"rows": lax.rem(me + p, n)}, device_id_type=MESH
            )

    @pl.when(me == 0)
    def _():
        for p in range(1, wide):
            pl.semaphore_signal(
                barrier, inc=1, device_id={"width": lax.rem(col + p, wide)}, device_id_type=MESH
            )

    heard = jnp.where(me < 2, min(n, NEAR) - 1, n - 1) + jnp.where(me == 0, wide - 1, 0)
    ahead = min(AHEAD, len(chunks))
    for k in range(3):
        load_top(k).start()
    for j in range(ahead):
        for k in range(3):
            load(j, k).start()
    for k in range(2):
        pltpu.make_async_copy(norms[k], gain.at[k], gain_sem.at[k]).start()

    def rows_of(j, low, high, acc):
        a, c, cw = chunks[j]
        weight, moment, square = held[a]
        cols = pl.ds(c, cw)

        def body(i, acc):
            rows = pl.ds(pl.multiple_of(i * block, block), block)
            w = weight[rows, cols]
            r = w - learn_rate * (
                moment[rows, cols] / (jnp.sqrt(square[rows, cols]) + tiny_value) + decay_rate * w
            )
            results[a][rows, cols] = r
            return acc + jnp.sum((r * r).reshape(block // 8, 8, cw), axis=0)

        return lax.fori_loop(low // block, high // block, body, acc)

    def update(j, low, acc):
        cw = chunks[j][2]
        for k in range(3):
            load(j, k).wait()
        if j + ahead < len(chunks):
            for k in range(3):
                load(j + ahead, k).start()
        acc = rows_of(j, low, depth, acc)
        sums[j, me, :, pl.ds(0, cw)] = jnp.sum(acc, axis=0, keepdims=True)

    def sum_copy(j, p, slot):
        return pltpu.make_async_remote_copy(
            src_ref=sums.at[j, me], dst_ref=sums.at[j, slot],
            send_sem=sum_send.at[j, p], recv_sem=sum_recv.at[j, p],
            device_id={"rows": lax.rem(me + p, n)}, device_id_type=MESH,
        )

    def norm_copy(slot):
        return pltpu.make_async_remote_copy(
            src_ref=own, dst_ref=serve.at[slot, col],
            send_sem=norm_send, recv_sem=norm_recv.at[slot],
            device_id={"rows": 0}, device_id_type=MESH,
        )

    def wide_copy(p, slot):
        return pltpu.make_async_remote_copy(
            src_ref=serve.at[:, col], dst_ref=serve.at[:, slot],
            send_sem=wide_send.at[p], recv_sem=wide_recv.at[p],
            device_id={"width": lax.rem(col + p, wide)}, device_id_type=MESH,
        )

    def serve_copy(row):
        return pltpu.make_async_remote_copy(
            src_ref=serve, dst_ref=serve,
            send_sem=serve_send.at[row], recv_sem=serve_recv,
            device_id={"rows": row}, device_id_type=MESH,
        )

    has_next = (me < n - 1, me > 0)
    step = (1, -1)
    keeps = (late & (me == n - 2), late & (me == 1))
    lacks = (last, first)

    opens = ((me == n - 2), (me == 1))
    opened = ((me == n - 1), (me == 0))

    def raw_copy(d):
        return pltpu.make_async_remote_copy(
            src_ref=results[0].at[pl.ds(0, top), pl.ds(0, chunks[0][2])], dst_ref=raw,
            send_sem=raw_send.at[d], recv_sem=raw_recv.at[d],
            device_id={"rows": lax.rem(me + step[d] + n, n)}, device_id_type=MESH,
        )

    def pass_on(d, h, j, a, cols, origin, skip=0):
        rows = pl.ds(pl.multiple_of(origin * depth + skip, block), depth - skip)
        return pltpu.make_async_remote_copy(
            src_ref=finals[a].at[rows, cols], dst_ref=finals[a].at[rows, cols],
            send_sem=send.at[d, h, j], recv_sem=recv.at[d, h, j],
            device_id={"rows": lax.rem(me + step[d] + n, n)}, device_id_type=MESH,
        )

    def finish(j, ready):
        a, c, cw = chunks[j]
        cols = pl.ds(c, cw)
        for p in range(1, n):
            sum_copy(j, p, lax.rem(me - p + n, n)).wait_recv()
        if j == 0:
            for p in range(1, n):
                @pl.when(jnp.logical_not(near[p - 1]))
                def _(p=p):
                    for i in range(ready):
                        sum_copy(i, p, me).start()
        total = sums[j, 0, :, pl.ds(0, cw)]
        for p in range(1, n):
            total = total + sums[j, p, :, pl.ds(0, cw)]
        scale = jnp.sqrt(total)
        columns[a][:, cols] = scale
        inverse = 1.0 / scale

        def body(i, carry):
            rows = pl.ds(pl.multiple_of(i * block, block), block)
            mine = pl.ds(pl.multiple_of(me * depth + i * block, block), block)
            finals[a][mine, cols] = (results[a][rows, cols] * inverse).astype(jnp.bfloat16)
            return carry

        lax.fori_loop(0, depth // block, body, 0)
        for d in (0, 1):
            goes = has_next[d]
            if a == 0 and j >= split:
                goes = goes & jnp.logical_not(keeps[d])
            if j == 0:
                goes = goes & jnp.logical_not(opens[d])
                pl.when(opens[d])(pass_on(d, 0, j, a, cols, me, top).start)

            @pl.when(goes)
            def _(d=d):
                pass_on(d, 0, j, a, cols, me).start()

    ready = 0
    for j in range(len(chunks)):
        while ready < min(len(chunks), LEAD * (j + 1)):
            acc, low = jnp.zeros((8, chunks[ready][2]), jnp.float32), 0
            if ready == 0:
                low = top
                for k in range(3):
                    load_top(k).wait()
                acc = rows_of(0, 0, top, acc)
                pl.semaphore_wait(barrier, heard)
                for d in (0, 1):
                    pl.when(opens[d])(raw_copy(d).start)
            update(ready, low, acc)
            for p in range(1, n):
                send_sum = sum_copy(ready, p, me).start
                if j == 0:
                    pl.when(near[p - 1])(send_sum)
                else:
                    send_sum()
            ready += 1
        finish(j, ready)

    for k in range(2):
        pltpu.make_async_copy(norms[k], gain.at[k], gain_sem.at[k]).wait()
    own[...] = (gain[0] + gain[1]).astype(jnp.bfloat16)

    @pl.when(me == 0)
    def _():
        serve[0, col] = own[...]

    @pl.when(me > 0)
    def _():
        norm_copy(me).start()

    for d in (0, 1):
        @pl.when(opened[d])
        def _(d=d):
            raw_copy(d).wait_recv()
            cw = chunks[0][2]
            inverse = 1.0 / columns[0][:, pl.ds(0, cw)]
            origin = (n - 2, 1)[d] * depth

            def body(i, carry):
                rows = pl.ds(pl.multiple_of(i * block, block), block)
                theirs = pl.ds(pl.multiple_of(origin + i * block, block), block)
                finals[0][theirs, pl.ds(0, cw)] = (raw[rows, :] * inverse).astype(jnp.bfloat16)
                return carry

            lax.fori_loop(0, top // block, body, 0)

    def span(a, cut, visit):
        cw = chunks[bases[a]][2]

        def body(k, carry):
            start = pl.multiple_of(k * cw, 128) if counts[a] > 1 else 0
            visit(bases[a] + k, a, pl.ds(start, cw))
            return carry

        low, high = cut
        if counts[a] > 1:
            lax.fori_loop(low, high, body, 0)
        elif high > low:
            body(0, 0)

    whole, tail, head = range(3)

    def parts(a, h):
        if a == 0 and h == 0:
            return ((0, 1), head), ((1, split), whole), ((split, counts[0]), tail)
        return (((0, counts[a]), whole),)

    def relay(h):
        for a in range(3):
            for cut, kind in parts(a, h):

                def visit(j, a, cols, kind=kind):
                    for d in (0, 1):
                        origin = me - step[d] * (h + 1)
                        comes = (origin >= 0) & (origin < n)
                        if kind == tail:
                            comes = comes & jnp.logical_not(lacks[d])
                        if kind == head:
                            comes = comes & jnp.logical_not(opened[d])
                            pl.when(opened[d])(
                                pass_on(d, h, j, a, cols, origin, top).wait_recv
                            )

                        @pl.when(comes)
                        def _(d=d, origin=origin):
                            pass_on(d, h, j, a, cols, origin).wait_recv()

                            if h + 1 < n - 1:
                                @pl.when(has_next[d])
                                def _():
                                    pass_on(d, h + 1, j, a, cols, origin).start()

                span(a, cut, visit)

    def drain(h):
        for d in (0, 1):
            origin = me - step[d] * h
            for a in range(3):
                for cut, kind in parts(a, h):
                    went = has_next[d] & (origin >= 0) & (origin < n)
                    if kind == tail:
                        went = went & jnp.logical_not(keeps[d])
                    if kind == head:
                        went = went & jnp.logical_not(opens[d])

                        @pl.when(opens[d])
                        def _(d=d):
                            raw_copy(d).wait_send()
                            cols = pl.ds(0, chunks[0][2])
                            pass_on(d, 0, 0, 0, cols, me, top).wait_send()

                    @pl.when(went)
                    def _(d=d, a=a, cut=cut, origin=origin):
                        span(
                            a, cut,
                            lambda j, a, cols: pass_on(d, h, j, a, cols, origin).wait_send(),
                        )

    for h in range(n - 1):
        if h == n - 2:
            for j in range(len(chunks)):
                for p in range(1, n):
                    sum_copy(j, p, me).wait_send()

            @pl.when(me > 0)
            def _():
                norm_copy(me).wait_send()
        relay(h)
        if h == 0:
            @pl.when(me == 0)
            def _():
                for row in range(1, n):
                    norm_copy(row).wait_recv()
                for p in range(1, wide):
                    wide_copy(p, col).start()
                for p in range(1, wide):
                    wide_copy(p, lax.rem(col - p + wide, wide)).wait_recv()
                for row in range(1, n):
                    serve_copy(row).start()
                for p in range(1, wide):
                    wide_copy(p, col).wait_send()
                for row in range(1, n):
                    serve_copy(row).wait_send()
        if h >= 1:
            drain(h - 1)
    drain(n - 2)

    @pl.when(me > 0)
    def _():
        serve_copy(0).wait_recv()


def store(n, site, kept, *refs):
    count = 10
    sources, targets = refs[:count], refs[count : 2 * count]
    handed, sem = refs[2 * count :]
    me, first, last = waits(n, site)
    depth, width = sources[0].shape[0] // n, sources[0].shape[1]
    copies = []
    for k in range(1, count):
        copies.append(pltpu.make_async_copy(sources[k], targets[k], sem.at[len(copies)]))
    maybe = []
    for o in range(n):
        rows = pl.ds(o * depth, depth)
        if kept < width:
            part = (rows, pl.ds(0, width - kept))
            copies.append(
                pltpu.make_async_copy(
                    sources[0].at[part], targets[0].at[part], sem.at[len(copies)]
                )
            )
        lacks = jnp.bool_(False)
        if o == 1:
            lacks = lacks | first
        if o == n - 2:
            lacks = lacks | last
        part = (rows, pl.ds(width - kept, kept))
        maybe.append(
            (
                jnp.logical_not(lacks),
                pltpu.make_async_copy(
                    sources[0].at[part], targets[0].at[part], sem.at[count - 1 + n + o]
                ),
            )
        )
    for copy in copies:
        copy.start()
    for has, copy in maybe:
        pl.when(has)(copy.start)
    handed[...] = sources[3][...]
    for copy in copies:
        copy.wait()
    for has, copy in maybe:
        pl.when(has)(copy.wait)


def finish_gather(n, site, final, after, piece, send, recv):
    me, first, last = waits(n, site)
    late = lax.axis_index("site") == site - 1
    depth, kept = piece.shape
    width = final.shape[1]
    keeps = (late & (me == n - 2), late & (me == 1))
    lacks = (last, first)
    step = (1, -1)

    barrier = pltpu.get_barrier_semaphore()
    count = jnp.int32(0)
    for d in (0, 1):
        for has, way in ((keeps[d], step[d]), (lacks[d], -step[d])):
            count = count + has.astype(jnp.int32)

            @pl.when(has)
            def _(way=way):
                pl.semaphore_signal(
                    barrier, inc=1, device_id={"rows": lax.rem(me + way + n, n)},
                    device_id_type=MESH,
                )

    @pl.when(count > 0)
    def _():
        pl.semaphore_wait(barrier, count)

    def tail(d):
        rows = pl.ds(pl.multiple_of(me * depth, depth), depth)
        return pltpu.make_async_remote_copy(
            src_ref=final.at[rows, pl.ds(width - kept, kept)], dst_ref=piece,
            send_sem=send.at[d], recv_sem=recv.at[d],
            device_id={"rows": lax.rem(me + step[d] + n, n)}, device_id_type=MESH,
        )

    for d in (0, 1):
        pl.when(keeps[d])(tail(d).start)
    for d in (0, 1):
        pl.when(keeps[d])(tail(d).wait_send)
        pl.when(lacks[d])(tail(d).wait_recv)


def finish_store(n, site, query, piece, out, sem):
    me, first, last = waits(n, site)
    depth, kept = piece.shape
    width = out.shape[1]
    for has, origin in ((first, 1), (last, n - 2)):
        part = (pl.ds(origin * depth, depth), pl.ds(width - kept, kept))

        @pl.when(has)
        def _(part=part):
            copy = pltpu.make_async_copy(piece, out.at[part], sem)
            copy.start()
            copy.wait()


def solution(mesh):
    n, wide, site = mesh.shape["rows"], mesh.shape["width"], mesh.shape["site"]

    def per_device(*args):
        arrays, (norm_train, norm_step) = args[:9], args[9:]
        depth = arrays[0].shape[0]
        widths = [arrays[3 * a].shape[1] for a in range(3)]
        chunks = chunks_of(widths)
        count = len(chunks)
        kept = widths[0] - chunks[late_of(chunks)][1]
        part = norm_train.shape[0]
        lanes = 128 if part % 128 == 0 else part
        norms = [x.reshape(part // lanes, lanes) for x in (norm_train, norm_step)]
        vmem, dma, hbm = pltpu.VMEM, pltpu.SemaphoreType.DMA, pltpu.HBM
        in_vmem, in_hbm = pl.BlockSpec(memory_space=vmem), pl.BlockSpec(memory_space=hbm)

        def pinned(x):
            return pltpu.with_memory_space_constraint(x, vmem)

        def shaped(x):
            return jax.ShapeDtypeStruct(x.shape, x.dtype)

        out_shape = (
            [vmem((n * depth, w), jnp.bfloat16) for w in widths]
            + [vmem((1, w), jnp.float32) for w in widths]
            + [vmem((n, wide, part // lanes, lanes), jnp.bfloat16)]
            + [vmem((depth, w), jnp.float32) for w in widths]
        )
        padded = sum(-(-w // 128) * 128 for w in widths)
        outside = padded * depth * (2 * n + 4) + (1 << 20)
        outs = pl.pallas_call(
            functools.partial(gather, n, wide, site, chunks),
            out_shape=out_shape,
            in_specs=[in_hbm] * 11,
            out_specs=[in_vmem] * 10,
            scratch_shapes=[vmem((depth, w), jnp.float32) for w in widths for _ in range(3)]
            + [
                vmem((2, part // lanes, lanes), jnp.float32),
                vmem((count, n, 1, 128), jnp.float32),
                dma((count, 3)),
                dma((2,)),
                dma((count, n)),
                dma((count, n)),
                dma((2, n - 1, count)),
                dma((2, n - 1, count)),
                dma,
                dma((n,)),
                dma((wide,)),
                dma((wide,)),
                vmem((head_of(depth, block_of(depth)), chunks[0][2]), jnp.float32),
                dma((3,)),
                dma((2,)),
                dma((2,)),
                vmem((part // lanes, lanes), jnp.bfloat16),
                dma((n,)),
                dma,
            ],
            compiler_params=pltpu.CompilerParams(
                collective_id=0,
                has_side_effects=True,
                vmem_limit_bytes=60 * (1 << 20) - outside,
            ),
        )(*arrays, *norms)
        outs = [pinned(x) for x in outs]
        stored = pl.pallas_call(
            functools.partial(store, n, site, kept),
            out_shape=[shaped(x) for x in outs] + [out_shape[3]],
            in_specs=[in_vmem] * 10,
            out_specs=[in_hbm] * 10 + [in_vmem],
            scratch_shapes=[dma((9 + 2 * n,))],
            compiler_params=pltpu.CompilerParams(vmem_limit_bytes=1 << 20),
        )(*outs)
        piece = pl.pallas_call(
            functools.partial(finish_gather, n, site),
            out_shape=vmem((depth, kept), jnp.bfloat16),
            in_specs=[in_vmem] * 2,
            out_specs=in_vmem,
            scratch_shapes=[dma((2,)), dma((2,))],
            compiler_params=pltpu.CompilerParams(
                collective_id=1, has_side_effects=True, vmem_limit_bytes=1 << 20
            ),
        )(outs[0], pinned(stored[10]))
        query = pl.pallas_call(
            functools.partial(finish_store, n, site),
            out_shape=shaped(stored[0]),
            in_specs=[in_hbm, in_vmem],
            out_specs=in_hbm,
            scratch_shapes=[pltpu.SemaphoreType.DMA],
            input_output_aliases={0: 0},
            compiler_params=pltpu.CompilerParams(vmem_limit_bytes=1 << 20),
        )(stored[0], pinned(piece))
        return (
            query,
            *stored[1:3],
            *(c.reshape(-1) for c in stored[3:6]),
            stored[6].reshape(-1),
            *stored[7:10],
        )

    cut = P(("site", "rows"), "width")
    return jax.shard_map(
        per_device,
        mesh=mesh,
        in_specs=(cut,) * 9 + (P(("site", "rows", "width")),) * 2,
        out_specs=(P("site", "width"),) * 3
        + (P(("site", "width")),) * 3
        + (P("site"),)
        + (cut,) * 3,
        check_vma=False,
    )
```

```python
import functools

import jax
import jax.numpy as jnp
from jax import lax
from jax.experimental import pallas as pl
from jax.experimental.pallas import tpu as pltpu
from jax.sharding import PartitionSpec as P

learn_rate = 0.02
decay_rate = 0.05
tiny_value = 1e-08

LEAD = 4
AHEAD = 4
HELD = 4, 8
HEAD = 5, 16
NEAR = 3
MESH = pl.DeviceIdType.MESH


def chunks_of(widths):
    out = []
    for a, width in enumerate(widths):
        step = 128 if width % 128 == 0 else width
        out += [(a, c, step) for c in range(0, width, step)]
    return out


def late_of(chunks):
    count = sum(1 for ch in chunks if ch[0] == 0)
    return count - max(1, count * HELD[0] // HELD[1])


def head_of(depth, block):
    return block * max(1, depth // block * HEAD[0] // HEAD[1])


def block_of(depth):
    return min(depth, 64)


def waits(n, site):
    me = lax.axis_index("rows")
    late = lax.axis_index("site") == site - 1
    return me, late & (me == 0), late & (me == n - 1)


def gather(n, wide, site, chunks, *refs):
    inputs, norms = [refs[0:3], refs[3:6], refs[6:9]], refs[9:11]
    finals, columns, serve, results = refs[11:14], refs[14:17], refs[17], refs[18:21]
    held = [refs[21:24], refs[24:27], refs[27:30]]
    gain, sums, in_sem, gain_sem, sum_send, sum_recv, send, recv = refs[30:38]
    norm_send, norm_recv, wide_send, wide_recv, raw, top_sem, raw_send, raw_recv = refs[38:46]
    own, serve_send, serve_recv = refs[46:]
    me, first, last = waits(n, site)
    late = lax.axis_index("site") == site - 1
    col = lax.axis_index("width")
    depth = results[0].shape[0]
    block = block_of(depth)
    top = head_of(depth, block)
    split = late_of(chunks)
    counts = [sum(1 for ch in chunks if ch[0] == a) for a in range(3)]
    bases = [sum(counts[:a]) for a in range(3)]

    barrier = pltpu.get_barrier_semaphore()

    def load(j, k):
        a, c, cw = chunks[j]
        part = (pl.ds(0, depth) if j else pl.ds(top, depth - top), pl.ds(c, cw))
        return pltpu.make_async_copy(
            inputs[a][k].at[part], held[a][k].at[part], in_sem.at[j, k]
        )

    def load_top(k):
        part = (pl.ds(0, top), pl.ds(0, chunks[0][2]))
        return pltpu.make_async_copy(inputs[0][k].at[part], held[0][k].at[part], top_sem.at[k])

    for k in range(3):
        load_top(k).start()
    near = [
        jnp.logical_not((me < 2) & (lax.rem(me + p, n) >= NEAR - me)) for p in range(1, n)
    ]
    for p in range(1, n):
        to = lax.rem(me + p, n)

        @pl.when(jnp.logical_not((to < 2) & (me >= NEAR - to)))
        def _(p=p):
            pl.semaphore_signal(
                barrier, inc=1, device_id={"rows": lax.rem(me + p, n)}, device_id_type=MESH
            )

    @pl.when(me == 0)
    def _():
        for p in range(1, wide):
            pl.semaphore_signal(
                barrier, inc=1, device_id={"width": lax.rem(col + p, wide)}, device_id_type=MESH
            )

    heard = jnp.where(me == 0, min(n, NEAR) - 1, jnp.where(me == 1, 1, n - 1)) + jnp.where(me == 0, wide - 1, 0)
    ahead = min(AHEAD, len(chunks))
    for j in range(ahead):
        for k in range(3):
            load(j, k).start()
    for k in range(2):
        pltpu.make_async_copy(norms[k], gain.at[k], gain_sem.at[k]).start()

    def rows_of(j, low, high, acc):
        a, c, cw = chunks[j]
        weight, moment, square = held[a]
        cols = pl.ds(c, cw)

        def body(i, acc):
            rows = pl.ds(pl.multiple_of(i * block, block), block)
            w = weight[rows, cols]
            r = w - learn_rate * (
                moment[rows, cols] / (jnp.sqrt(square[rows, cols]) + tiny_value) + decay_rate * w
            )
            results[a][rows, cols] = r
            return acc + jnp.sum((r * r).reshape(block // 8, 8, cw), axis=0)

        return lax.fori_loop(low // block, high // block, body, acc)

    def update(j, low, acc):
        cw = chunks[j][2]
        for k in range(3):
            load(j, k).wait()
        if j + ahead < len(chunks):
            for k in range(3):
                load(j + ahead, k).start()
        acc = rows_of(j, low, depth, acc)
        sums[j, me, :, pl.ds(0, cw)] = jnp.sum(acc, axis=0, keepdims=True)

    def sum_copy(j, p, slot):
        return pltpu.make_async_remote_copy(
            src_ref=sums.at[j, me], dst_ref=sums.at[j, slot],
            send_sem=sum_send.at[j, p], recv_sem=sum_recv.at[j, p],
            device_id={"rows": lax.rem(me + p, n)}, device_id_type=MESH,
        )

    def norm_copy(slot):
        return pltpu.make_async_remote_copy(
            src_ref=own, dst_ref=serve.at[slot, col],
            send_sem=norm_send, recv_sem=norm_recv.at[slot],
            device_id={"rows": 0}, device_id_type=MESH,
        )

    def wide_copy(p, slot):
        return pltpu.make_async_remote_copy(
            src_ref=serve.at[:, col], dst_ref=serve.at[:, slot],
            send_sem=wide_send.at[p], recv_sem=wide_recv.at[p],
            device_id={"width": lax.rem(col + p, wide)}, device_id_type=MESH,
        )

    def serve_copy(row):
        return pltpu.make_async_remote_copy(
            src_ref=serve, dst_ref=serve,
            send_sem=serve_send.at[row], recv_sem=serve_recv,
            device_id={"rows": row}, device_id_type=MESH,
        )

    has_next = (me < n - 1, me > 0)
    step = (1, -1)
    keeps = (late & (me == n - 2), late & (me == 1))
    lacks = (last, first)

    opens = ((me == n - 2), (me == 1))
    opened = ((me == n - 1), (me == 0))

    def raw_copy(d):
        return pltpu.make_async_remote_copy(
            src_ref=results[0].at[pl.ds(0, top), pl.ds(0, chunks[0][2])], dst_ref=raw,
            send_sem=raw_send.at[d], recv_sem=raw_recv.at[d],
            device_id={"rows": lax.rem(me + step[d] + n, n)}, device_id_type=MESH,
        )

    def pass_on(d, h, j, a, cols, origin, skip=0):
        rows = pl.ds(pl.multiple_of(origin * depth + skip, block), depth - skip)
        return pltpu.make_async_remote_copy(
            src_ref=finals[a].at[rows, cols], dst_ref=finals[a].at[rows, cols],
            send_sem=send.at[d, h, j], recv_sem=recv.at[d, h, j],
            device_id={"rows": lax.rem(me + step[d] + n, n)}, device_id_type=MESH,
        )

    def finish(j, ready):
        a, c, cw = chunks[j]
        cols = pl.ds(c, cw)
        for p in range(1, n):
            sum_copy(j, p, lax.rem(me - p + n, n)).wait_recv()
        if j == 0:
            for p in range(1, n):
                @pl.when(jnp.logical_not(near[p - 1]))
                def _(p=p):
                    for i in range(ready):
                        sum_copy(i, p, me).start()
        total = sums[j, 0, :, pl.ds(0, cw)]
        for p in range(1, n):
            total = total + sums[j, p, :, pl.ds(0, cw)]
        scale = jnp.sqrt(total)
        columns[a][:, cols] = scale
        inverse = 1.0 / scale

        def body(i, carry):
            rows = pl.ds(pl.multiple_of(i * block, block), block)
            mine = pl.ds(pl.multiple_of(me * depth + i * block, block), block)
            finals[a][mine, cols] = (results[a][rows, cols] * inverse).astype(jnp.bfloat16)
            return carry

        lax.fori_loop(0, depth // block, body, 0)
        for d in (0, 1):
            goes = has_next[d]
            if a == 0 and j >= split:
                goes = goes & jnp.logical_not(keeps[d])
            if j == 0:
                goes = goes & jnp.logical_not(opens[d])
                pl.when(opens[d])(pass_on(d, 0, j, a, cols, me, top).start)

            @pl.when(goes)
            def _(d=d):
                pass_on(d, 0, j, a, cols, me).start()

    ready = 0
    for j in range(len(chunks)):
        while ready < min(len(chunks), LEAD * (j + 1)):
            acc, low = jnp.zeros((8, chunks[ready][2]), jnp.float32), 0
            if ready == 0:
                low = top
                for k in range(3):
                    load_top(k).wait()
                acc = rows_of(0, 0, top, acc)
                pl.semaphore_wait(barrier, heard)
                for d in (0, 1):
                    pl.when(opens[d])(raw_copy(d).start)
            update(ready, low, acc)
            for p in range(1, n):
                send_sum = sum_copy(ready, p, me).start
                if j == 0:
                    pl.when(near[p - 1])(send_sum)
                else:
                    send_sum()
            ready += 1
        finish(j, ready)

    for k in range(2):
        pltpu.make_async_copy(norms[k], gain.at[k], gain_sem.at[k]).wait()
    own[...] = (gain[0] + gain[1]).astype(jnp.bfloat16)

    @pl.when(me == 0)
    def _():
        serve[0, col] = own[...]

    @pl.when(me > 0)
    def _():
        norm_copy(me).start()

    for d in (0, 1):
        @pl.when(opened[d])
        def _(d=d):
            raw_copy(d).wait_recv()
            cw = chunks[0][2]
            inverse = 1.0 / columns[0][:, pl.ds(0, cw)]
            origin = (n - 2, 1)[d] * depth

            def body(i, carry):
                rows = pl.ds(pl.multiple_of(i * block, block), block)
                theirs = pl.ds(pl.multiple_of(origin + i * block, block), block)
                finals[0][theirs, pl.ds(0, cw)] = (raw[rows, :] * inverse).astype(jnp.bfloat16)
                return carry

            lax.fori_loop(0, top // block, body, 0)

    def span(a, cut, visit):
        cw = chunks[bases[a]][2]

        def body(k, carry):
            start = pl.multiple_of(k * cw, 128) if counts[a] > 1 else 0
            visit(bases[a] + k, a, pl.ds(start, cw))
            return carry

        low, high = cut
        if counts[a] > 1:
            lax.fori_loop(low, high, body, 0)
        elif high > low:
            body(0, 0)

    whole, tail, head = range(3)

    def parts(a, h):
        if a == 0 and h == 0:
            return ((0, 1), head), ((1, split), whole), ((split, counts[0]), tail)
        return (((0, counts[a]), whole),)

    def relay(h):
        for a in range(3):
            for cut, kind in parts(a, h):

                def visit(j, a, cols, kind=kind):
                    for d in (0, 1):
                        origin = me - step[d] * (h + 1)
                        comes = (origin >= 0) & (origin < n)
                        if kind == tail:
                            comes = comes & jnp.logical_not(lacks[d])
                        if kind == head:
                            comes = comes & jnp.logical_not(opened[d])
                            pl.when(opened[d])(
                                pass_on(d, h, j, a, cols, origin, top).wait_recv
                            )

                        @pl.when(comes)
                        def _(d=d, origin=origin):
                            pass_on(d, h, j, a, cols, origin).wait_recv()

                            if h + 1 < n - 1:
                                @pl.when(has_next[d])
                                def _():
                                    pass_on(d, h + 1, j, a, cols, origin).start()

                span(a, cut, visit)

    def drain(h):
        for d in (0, 1):
            origin = me - step[d] * h
            for a in range(3):
                for cut, kind in parts(a, h):
                    went = has_next[d] & (origin >= 0) & (origin < n)
                    if kind == tail:
                        went = went & jnp.logical_not(keeps[d])
                    if kind == head:
                        went = went & jnp.logical_not(opens[d])

                        @pl.when(opens[d])
                        def _(d=d):
                            raw_copy(d).wait_send()
                            cols = pl.ds(0, chunks[0][2])
                            pass_on(d, 0, 0, 0, cols, me, top).wait_send()

                    @pl.when(went)
                    def _(d=d, a=a, cut=cut, origin=origin):
                        span(
                            a, cut,
                            lambda j, a, cols: pass_on(d, h, j, a, cols, origin).wait_send(),
                        )

    for h in range(n - 1):
        if h == n - 2:
            for j in range(len(chunks)):
                for p in range(1, n):
                    sum_copy(j, p, me).wait_send()

            @pl.when(me > 0)
            def _():
                norm_copy(me).wait_send()
        relay(h)
        if h == 0:
            @pl.when(me == 0)
            def _():
                for row in range(1, n):
                    norm_copy(row).wait_recv()
                for p in range(1, wide):
                    wide_copy(p, col).start()
                for p in range(1, wide):
                    wide_copy(p, lax.rem(col - p + wide, wide)).wait_recv()
                for row in range(1, n):
                    serve_copy(row).start()
                for p in range(1, wide):
                    wide_copy(p, col).wait_send()
                for row in range(1, n):
                    serve_copy(row).wait_send()
        if h >= 1:
            drain(h - 1)
    drain(n - 2)

    @pl.when(me > 0)
    def _():
        serve_copy(0).wait_recv()


def store(n, site, kept, *refs):
    count = 10
    sources, targets = refs[:count], refs[count : 2 * count]
    handed, sem = refs[2 * count :]
    me, first, last = waits(n, site)
    depth, width = sources[0].shape[0] // n, sources[0].shape[1]
    copies = []
    for k in range(1, count):
        copies.append(pltpu.make_async_copy(sources[k], targets[k], sem.at[len(copies)]))
    maybe = []
    for o in range(n):
        rows = pl.ds(o * depth, depth)
        if kept < width:
            part = (rows, pl.ds(0, width - kept))
            copies.append(
                pltpu.make_async_copy(
                    sources[0].at[part], targets[0].at[part], sem.at[len(copies)]
                )
            )
        lacks = jnp.bool_(False)
        if o == 1:
            lacks = lacks | first
        if o == n - 2:
            lacks = lacks | last
        part = (rows, pl.ds(width - kept, kept))
        maybe.append(
            (
                jnp.logical_not(lacks),
                pltpu.make_async_copy(
                    sources[0].at[part], targets[0].at[part], sem.at[count - 1 + n + o]
                ),
            )
        )
    for copy in copies:
        copy.start()
    for has, copy in maybe:
        pl.when(has)(copy.start)
    handed[...] = sources[3][...]
    for copy in copies:
        copy.wait()
    for has, copy in maybe:
        pl.when(has)(copy.wait)


def finish_gather(n, site, final, after, piece, send, recv):
    me, first, last = waits(n, site)
    late = lax.axis_index("site") == site - 1
    depth, kept = piece.shape
    width = final.shape[1]
    keeps = (late & (me == n - 2), late & (me == 1))
    lacks = (last, first)
    step = (1, -1)

    barrier = pltpu.get_barrier_semaphore()
    count = jnp.int32(0)
    for d in (0, 1):
        for has, way in ((keeps[d], step[d]), (lacks[d], -step[d])):
            count = count + has.astype(jnp.int32)

            @pl.when(has)
            def _(way=way):
                pl.semaphore_signal(
                    barrier, inc=1, device_id={"rows": lax.rem(me + way + n, n)},
                    device_id_type=MESH,
                )

    @pl.when(count > 0)
    def _():
        pl.semaphore_wait(barrier, count)

    def tail(d):
        rows = pl.ds(pl.multiple_of(me * depth, depth), depth)
        return pltpu.make_async_remote_copy(
            src_ref=final.at[rows, pl.ds(width - kept, kept)], dst_ref=piece,
            send_sem=send.at[d], recv_sem=recv.at[d],
            device_id={"rows": lax.rem(me + step[d] + n, n)}, device_id_type=MESH,
        )

    for d in (0, 1):
        pl.when(keeps[d])(tail(d).start)
    for d in (0, 1):
        pl.when(keeps[d])(tail(d).wait_send)
        pl.when(lacks[d])(tail(d).wait_recv)


def finish_store(n, site, query, piece, out, sem):
    me, first, last = waits(n, site)
    depth, kept = piece.shape
    width = out.shape[1]
    for has, origin in ((first, 1), (last, n - 2)):
        part = (pl.ds(origin * depth, depth), pl.ds(width - kept, kept))

        @pl.when(has)
        def _(part=part):
            copy = pltpu.make_async_copy(piece, out.at[part], sem)
            copy.start()
            copy.wait()


def solution(mesh):
    n, wide, site = mesh.shape["rows"], mesh.shape["width"], mesh.shape["site"]

    def per_device(*args):
        arrays, (norm_train, norm_step) = args[:9], args[9:]
        depth = arrays[0].shape[0]
        widths = [arrays[3 * a].shape[1] for a in range(3)]
        chunks = chunks_of(widths)
        count = len(chunks)
        kept = widths[0] - chunks[late_of(chunks)][1]
        part = norm_train.shape[0]
        lanes = 128 if part % 128 == 0 else part
        norms = [x.reshape(part // lanes, lanes) for x in (norm_train, norm_step)]
        vmem, dma, hbm = pltpu.VMEM, pltpu.SemaphoreType.DMA, pltpu.HBM
        in_vmem, in_hbm = pl.BlockSpec(memory_space=vmem), pl.BlockSpec(memory_space=hbm)

        def pinned(x):
            return pltpu.with_memory_space_constraint(x, vmem)

        def shaped(x):
            return jax.ShapeDtypeStruct(x.shape, x.dtype)

        out_shape = (
            [vmem((n * depth, w), jnp.bfloat16) for w in widths]
            + [vmem((1, w), jnp.float32) for w in widths]
            + [vmem((n, wide, part // lanes, lanes), jnp.bfloat16)]
            + [vmem((depth, w), jnp.float32) for w in widths]
        )
        padded = sum(-(-w // 128) * 128 for w in widths)
        outside = padded * depth * (2 * n + 4) + (1 << 20)
        outs = pl.pallas_call(
            functools.partial(gather, n, wide, site, chunks),
            out_shape=out_shape,
            in_specs=[in_hbm] * 11,
            out_specs=[in_vmem] * 10,
            scratch_shapes=[vmem((depth, w), jnp.float32) for w in widths for _ in range(3)]
            + [
                vmem((2, part // lanes, lanes), jnp.float32),
                vmem((count, n, 1, 128), jnp.float32),
                dma((count, 3)),
                dma((2,)),
                dma((count, n)),
                dma((count, n)),
                dma((2, n - 1, count)),
                dma((2, n - 1, count)),
                dma,
                dma((n,)),
                dma((wide,)),
                dma((wide,)),
                vmem((head_of(depth, block_of(depth)), chunks[0][2]), jnp.float32),
                dma((3,)),
                dma((2,)),
                dma((2,)),
                vmem((part // lanes, lanes), jnp.bfloat16),
                dma((n,)),
                dma,
            ],
            compiler_params=pltpu.CompilerParams(
                collective_id=0,
                has_side_effects=True,
                vmem_limit_bytes=60 * (1 << 20) - outside,
            ),
        )(*arrays, *norms)
        outs = [pinned(x) for x in outs]
        stored = pl.pallas_call(
            functools.partial(store, n, site, kept),
            out_shape=[shaped(x) for x in outs] + [out_shape[3]],
            in_specs=[in_vmem] * 10,
            out_specs=[in_hbm] * 10 + [in_vmem],
            scratch_shapes=[dma((9 + 2 * n,))],
            compiler_params=pltpu.CompilerParams(vmem_limit_bytes=1 << 20),
        )(*outs)
        piece = pl.pallas_call(
            functools.partial(finish_gather, n, site),
            out_shape=vmem((depth, kept), jnp.bfloat16),
            in_specs=[in_vmem] * 2,
            out_specs=in_vmem,
            scratch_shapes=[dma((2,)), dma((2,))],
            compiler_params=pltpu.CompilerParams(
                collective_id=1, has_side_effects=True, vmem_limit_bytes=1 << 20
            ),
        )(outs[0], pinned(stored[10]))
        query = pl.pallas_call(
            functools.partial(finish_store, n, site),
            out_shape=shaped(stored[0]),
            in_specs=[in_hbm, in_vmem],
            out_specs=in_hbm,
            scratch_shapes=[pltpu.SemaphoreType.DMA],
            input_output_aliases={0: 0},
            compiler_params=pltpu.CompilerParams(vmem_limit_bytes=1 << 20),
        )(stored[0], pinned(piece))
        return (
            query,
            *stored[1:3],
            *(c.reshape(-1) for c in stored[3:6]),
            stored[6].reshape(-1),
            *stored[7:10],
        )

    cut = P(("site", "rows"), "width")
    return jax.shard_map(
        per_device,
        mesh=mesh,
        in_specs=(cut,) * 9 + (P(("site", "rows", "width")),) * 2,
        out_specs=(P("site", "width"),) * 3
        + (P(("site", "width")),) * 3
        + (P("site"),)
        + (cut,) * 3,
        check_vma=False,
    )
```

```python
import functools

import jax
import jax.numpy as jnp
from jax import lax
from jax.experimental import pallas as pl
from jax.experimental.pallas import tpu as pltpu
from jax.sharding import PartitionSpec as P

learn_rate = 0.02
decay_rate = 0.05
tiny_value = 1e-08

LEAD = 4
AHEAD = 4
HELD = 4, 8
HEAD = 6, 16
NEAR = 3
MESH = pl.DeviceIdType.MESH


def chunks_of(widths):
    out = []
    for a, width in enumerate(widths):
        step = 128 if width % 128 == 0 else width
        out += [(a, c, step) for c in range(0, width, step)]
    return out


def late_of(chunks):
    count = sum(1 for ch in chunks if ch[0] == 0)
    return count - max(1, count * HELD[0] // HELD[1])


def head_of(depth, block):
    return block * max(1, depth // block * HEAD[0] // HEAD[1])


def block_of(depth):
    return min(depth, 128)


def waits(n, site):
    me = lax.axis_index("rows")
    late = lax.axis_index("site") == site - 1
    return me, late & (me == 0), late & (me == n - 1)


def gather(n, wide, site, chunks, *refs):
    inputs, norms = [refs[0:3], refs[3:6], refs[6:9]], refs[9:11]
    finals, columns, serve, results = refs[11:14], refs[14:17], refs[17], refs[18:21]
    held = [refs[21:24], refs[24:27], refs[27:30]]
    gain, sums, in_sem, gain_sem, sum_send, sum_recv, send, recv = refs[30:38]
    norm_send, norm_recv, wide_send, wide_recv, raw, top_sem, raw_send, raw_recv = refs[38:46]
    own, serve_send, serve_recv = refs[46:]
    me, first, last = waits(n, site)
    late = lax.axis_index("site") == site - 1
    col = lax.axis_index("width")
    depth = results[0].shape[0]
    block = block_of(depth)
    top = head_of(depth, block)
    split = late_of(chunks)
    counts = [sum(1 for ch in chunks if ch[0] == a) for a in range(3)]
    bases = [sum(counts[:a]) for a in range(3)]

    barrier = pltpu.get_barrier_semaphore()

    def load(j, k):
        a, c, cw = chunks[j]
        part = (pl.ds(0, depth) if j else pl.ds(top, depth - top), pl.ds(c, cw))
        return pltpu.make_async_copy(
            inputs[a][k].at[part], held[a][k].at[part], in_sem.at[j, k]
        )

    def load_top(k):
        part = (pl.ds(0, top), pl.ds(0, chunks[0][2]))
        return pltpu.make_async_copy(inputs[0][k].at[part], held[0][k].at[part], top_sem.at[k])

    near = [
        jnp.logical_not((me < 2) & (lax.rem(me + p, n) >= NEAR)) for p in range(1, n)
    ]
    for p in range(1, n):
        @pl.when(jnp.logical_not((me >= NEAR) & (lax.rem(me + p, n) < 2)))
        def _(p=p):
            pl.semaphore_signal(
                barrier, inc=1, device_id={"rows": lax.rem(me + p, n)}, device_id_type=MESH
            )

    @pl.when(me == 0)
    def _():
        for p in range(1, wide):
            pl.semaphore_signal(
                barrier, inc=1, device_id={"width": lax.rem(col + p, wide)}, device_id_type=MESH
            )

    heard = jnp.where(me < 2, min(n, NEAR) - 1, n - 1) + jnp.where(me == 0, wide - 1, 0)
    ahead = min(AHEAD, len(chunks))
    for k in range(3):
        load_top(k).start()
    for j in range(ahead):
        for k in range(3):
            load(j, k).start()
    for k in range(2):
        pltpu.make_async_copy(norms[k], gain.at[k], gain_sem.at[k]).start()

    def rows_of(j, low, high, acc):
        a, c, cw = chunks[j]
        weight, moment, square = held[a]
        cols = pl.ds(c, cw)

        def body(i, acc):
            rows = pl.ds(pl.multiple_of(i * block, block), block)
            w = weight[rows, cols]
            r = w - learn_rate * (
                moment[rows, cols] / (jnp.sqrt(square[rows, cols]) + tiny_value) + decay_rate * w
            )
            results[a][rows, cols] = r
            return acc + jnp.sum((r * r).reshape(block // 8, 8, cw), axis=0)

        return lax.fori_loop(low // block, high // block, body, acc)

    def update(j, low, acc):
        cw = chunks[j][2]
        for k in range(3):
            load(j, k).wait()
        if j + ahead < len(chunks):
            for k in range(3):
                load(j + ahead, k).start()
        acc = rows_of(j, low, depth, acc)
        sums[j, me, :, pl.ds(0, cw)] = jnp.sum(acc, axis=0, keepdims=True)

    def sum_copy(j, p, slot):
        return pltpu.make_async_remote_copy(
            src_ref=sums.at[j, me], dst_ref=sums.at[j, slot],
            send_sem=sum_send.at[j, p], recv_sem=sum_recv.at[j, p],
            device_id={"rows": lax.rem(me + p, n)}, device_id_type=MESH,
        )

    def norm_copy(slot):
        return pltpu.make_async_remote_copy(
            src_ref=own, dst_ref=serve.at[slot, col],
            send_sem=norm_send, recv_sem=norm_recv.at[slot],
            device_id={"rows": 0}, device_id_type=MESH,
        )

    def wide_copy(p, slot):
        return pltpu.make_async_remote_copy(
            src_ref=serve.at[:, col], dst_ref=serve.at[:, slot],
            send_sem=wide_send.at[p], recv_sem=wide_recv.at[p],
            device_id={"width": lax.rem(col + p, wide)}, device_id_type=MESH,
        )

    def serve_copy(row):
        return pltpu.make_async_remote_copy(
            src_ref=serve, dst_ref=serve,
            send_sem=serve_send.at[row], recv_sem=serve_recv,
            device_id={"rows": row}, device_id_type=MESH,
        )

    has_next = (me < n - 1, me > 0)
    step = (1, -1)
    keeps = (late & (me == n - 2), late & (me == 1))
    lacks = (last, first)

    opens = ((me == n - 2), (me == 1))
    opened = ((me == n - 1), (me == 0))

    def raw_copy(d):
        return pltpu.make_async_remote_copy(
            src_ref=results[0].at[pl.ds(0, top), pl.ds(0, chunks[0][2])], dst_ref=raw,
            send_sem=raw_send.at[d], recv_sem=raw_recv.at[d],
            device_id={"rows": lax.rem(me + step[d] + n, n)}, device_id_type=MESH,
        )

    def pass_on(d, h, j, a, cols, origin, skip=0):
        rows = pl.ds(pl.multiple_of(origin * depth + skip, block), depth - skip)
        return pltpu.make_async_remote_copy(
            src_ref=finals[a].at[rows, cols], dst_ref=finals[a].at[rows, cols],
            send_sem=send.at[d, h, j], recv_sem=recv.at[d, h, j],
            device_id={"rows": lax.rem(me + step[d] + n, n)}, device_id_type=MESH,
        )

    def finish(j, ready):
        a, c, cw = chunks[j]
        cols = pl.ds(c, cw)
        for p in range(1, n):
            sum_copy(j, p, lax.rem(me - p + n, n)).wait_recv()
        if j == 0:
            for p in range(1, n):
                @pl.when(jnp.logical_not(near[p - 1]))
                def _(p=p):
                    for i in range(ready):
                        sum_copy(i, p, me).start()
        total = sums[j, 0, :, pl.ds(0, cw)]
        for p in range(1, n):
            total = total + sums[j, p, :, pl.ds(0, cw)]
        scale = jnp.sqrt(total)
        columns[a][:, cols] = scale
        inverse = 1.0 / scale

        def body(i, carry):
            rows = pl.ds(pl.multiple_of(i * block, block), block)
            mine = pl.ds(pl.multiple_of(me * depth + i * block, block), block)
            finals[a][mine, cols] = (results[a][rows, cols] * inverse).astype(jnp.bfloat16)
            return carry

        lax.fori_loop(0, depth // block, body, 0)
        for d in (0, 1):
            goes = has_next[d]
            if a == 0 and j >= split:
                goes = goes & jnp.logical_not(keeps[d])
            if j == 0:
                goes = goes & jnp.logical_not(opens[d])
                pl.when(opens[d])(pass_on(d, 0, j, a, cols, me, top).start)

            @pl.when(goes)
            def _(d=d):
                pass_on(d, 0, j, a, cols, me).start()

    ready = 0
    for j in range(len(chunks)):
        while ready < min(len(chunks), LEAD * (j + 1)):
            acc, low = jnp.zeros((8, chunks[ready][2]), jnp.float32), 0
            if ready == 0:
                low = top
                for k in range(3):
                    load_top(k).wait()
                acc = rows_of(0, 0, top, acc)
                pl.semaphore_wait(barrier, heard)
                for d in (0, 1):
                    pl.when(opens[d])(raw_copy(d).start)
            update(ready, low, acc)
            for p in range(1, n):
                send_sum = sum_copy(ready, p, me).start
                if j == 0:
                    pl.when(near[p - 1])(send_sum)
                else:
                    send_sum()
            ready += 1
        finish(j, ready)

    for k in range(2):
        pltpu.make_async_copy(norms[k], gain.at[k], gain_sem.at[k]).wait()
    own[...] = (gain[0] + gain[1]).astype(jnp.bfloat16)

    @pl.when(me == 0)
    def _():
        serve[0, col] = own[...]

    @pl.when(me > 0)
    def _():
        norm_copy(me).start()

    for d in (0, 1):
        @pl.when(opened[d])
        def _(d=d):
            raw_copy(d).wait_recv()
            cw = chunks[0][2]
            inverse = 1.0 / columns[0][:, pl.ds(0, cw)]
            origin = (n - 2, 1)[d] * depth

            def body(i, carry):
                rows = pl.ds(pl.multiple_of(i * block, block), block)
                theirs = pl.ds(pl.multiple_of(origin + i * block, block), block)
                finals[0][theirs, pl.ds(0, cw)] = (raw[rows, :] * inverse).astype(jnp.bfloat16)
                return carry

            lax.fori_loop(0, top // block, body, 0)

    def span(a, cut, visit):
        cw = chunks[bases[a]][2]

        def body(k, carry):
            start = pl.multiple_of(k * cw, 128) if counts[a] > 1 else 0
            visit(bases[a] + k, a, pl.ds(start, cw))
            return carry

        low, high = cut
        if counts[a] > 1:
            lax.fori_loop(low, high, body, 0)
        elif high > low:
            body(0, 0)

    whole, tail, head = range(3)

    def parts(a, h):
        if a == 0 and h == 0:
            return ((0, 1), head), ((1, split), whole), ((split, counts[0]), tail)
        return (((0, counts[a]), whole),)

    def relay(h):
        for a in range(3):
            for cut, kind in parts(a, h):

                def visit(j, a, cols, kind=kind):
                    for d in (0, 1):
                        origin = me - step[d] * (h + 1)
                        comes = (origin >= 0) & (origin < n)
                        if kind == tail:
                            comes = comes & jnp.logical_not(lacks[d])
                        if kind == head:
                            comes = comes & jnp.logical_not(opened[d])
                            pl.when(opened[d])(
                                pass_on(d, h, j, a, cols, origin, top).wait_recv
                            )

                        @pl.when(comes)
                        def _(d=d, origin=origin):
                            pass_on(d, h, j, a, cols, origin).wait_recv()

                            if h + 1 < n - 1:
                                @pl.when(has_next[d])
                                def _():
                                    pass_on(d, h + 1, j, a, cols, origin).start()

                span(a, cut, visit)

    def drain(h):
        for d in (0, 1):
            origin = me - step[d] * h
            for a in range(3):
                for cut, kind in parts(a, h):
                    went = has_next[d] & (origin >= 0) & (origin < n)
                    if kind == tail:
                        went = went & jnp.logical_not(keeps[d])
                    if kind == head:
                        went = went & jnp.logical_not(opens[d])

                        @pl.when(opens[d])
                        def _(d=d):
                            raw_copy(d).wait_send()
                            cols = pl.ds(0, chunks[0][2])
                            pass_on(d, 0, 0, 0, cols, me, top).wait_send()

                    @pl.when(went)
                    def _(d=d, a=a, cut=cut, origin=origin):
                        span(
                            a, cut,
                            lambda j, a, cols: pass_on(d, h, j, a, cols, origin).wait_send(),
                        )

    for h in range(n - 1):
        if h == n - 2:
            for j in range(len(chunks)):
                for p in range(1, n):
                    sum_copy(j, p, me).wait_send()

            @pl.when(me > 0)
            def _():
                norm_copy(me).wait_send()
        relay(h)
        if h == 0:
            @pl.when(me == 0)
            def _():
                for row in range(1, n):
                    norm_copy(row).wait_recv()
                for p in range(1, wide):
                    wide_copy(p, col).start()
                for p in range(1, wide):
                    wide_copy(p, lax.rem(col - p + wide, wide)).wait_recv()
                for row in range(1, n):
                    serve_copy(row).start()
                for p in range(1, wide):
                    wide_copy(p, col).wait_send()
                for row in range(1, n):
                    serve_copy(row).wait_send()
        if h >= 1:
            drain(h - 1)
    drain(n - 2)

    @pl.when(me > 0)
    def _():
        serve_copy(0).wait_recv()


def store(n, site, kept, *refs):
    count = 10
    sources, targets = refs[:count], refs[count : 2 * count]
    handed, sem = refs[2 * count :]
    me, first, last = waits(n, site)
    depth, width = sources[0].shape[0] // n, sources[0].shape[1]
    copies = []
    for k in range(1, count):
        copies.append(pltpu.make_async_copy(sources[k], targets[k], sem.at[len(copies)]))
    maybe = []
    for o in range(n):
        rows = pl.ds(o * depth, depth)
        if kept < width:
            part = (rows, pl.ds(0, width - kept))
            copies.append(
                pltpu.make_async_copy(
                    sources[0].at[part], targets[0].at[part], sem.at[len(copies)]
                )
            )
        lacks = jnp.bool_(False)
        if o == 1:
            lacks = lacks | first
        if o == n - 2:
            lacks = lacks | last
        part = (rows, pl.ds(width - kept, kept))
        maybe.append(
            (
                jnp.logical_not(lacks),
                pltpu.make_async_copy(
                    sources[0].at[part], targets[0].at[part], sem.at[count - 1 + n + o]
                ),
            )
        )
    for copy in copies:
        copy.start()
    for has, copy in maybe:
        pl.when(has)(copy.start)
    handed[...] = sources[3][...]
    for copy in copies:
        copy.wait()
    for has, copy in maybe:
        pl.when(has)(copy.wait)


def finish_gather(n, site, final, after, piece, send, recv):
    me, first, last = waits(n, site)
    late = lax.axis_index("site") == site - 1
    depth, kept = piece.shape
    width = final.shape[1]
    keeps = (late & (me == n - 2), late & (me == 1))
    lacks = (last, first)
    step = (1, -1)

    barrier = pltpu.get_barrier_semaphore()
    count = jnp.int32(0)
    for d in (0, 1):
        for has, way in ((keeps[d], step[d]), (lacks[d], -step[d])):
            count = count + has.astype(jnp.int32)

            @pl.when(has)
            def _(way=way):
                pl.semaphore_signal(
                    barrier, inc=1, device_id={"rows": lax.rem(me + way + n, n)},
                    device_id_type=MESH,
                )

    @pl.when(count > 0)
    def _():
        pl.semaphore_wait(barrier, count)

    def tail(d):
        rows = pl.ds(pl.multiple_of(me * depth, depth), depth)
        return pltpu.make_async_remote_copy(
            src_ref=final.at[rows, pl.ds(width - kept, kept)], dst_ref=piece,
            send_sem=send.at[d], recv_sem=recv.at[d],
            device_id={"rows": lax.rem(me + step[d] + n, n)}, device_id_type=MESH,
        )

    for d in (0, 1):
        pl.when(keeps[d])(tail(d).start)
    for d in (0, 1):
        pl.when(keeps[d])(tail(d).wait_send)
        pl.when(lacks[d])(tail(d).wait_recv)


def finish_store(n, site, query, piece, out, sem):
    me, first, last = waits(n, site)
    depth, kept = piece.shape
    width = out.shape[1]
    for has, origin in ((first, 1), (last, n - 2)):
        part = (pl.ds(origin * depth, depth), pl.ds(width - kept, kept))

        @pl.when(has)
        def _(part=part):
            copy = pltpu.make_async_copy(piece, out.at[part], sem)
            copy.start()
            copy.wait()


def solution(mesh):
    n, wide, site = mesh.shape["rows"], mesh.shape["width"], mesh.shape["site"]

    def per_device(*args):
        arrays, (norm_train, norm_step) = args[:9], args[9:]
        depth = arrays[0].shape[0]
        widths = [arrays[3 * a].shape[1] for a in range(3)]
        chunks = chunks_of(widths)
        count = len(chunks)
        kept = widths[0] - chunks[late_of(chunks)][1]
        part = norm_train.shape[0]
        lanes = 128 if part % 128 == 0 else part
        norms = [x.reshape(part // lanes, lanes) for x in (norm_train, norm_step)]
        vmem, dma, hbm = pltpu.VMEM, pltpu.SemaphoreType.DMA, pltpu.HBM
        in_vmem, in_hbm = pl.BlockSpec(memory_space=vmem), pl.BlockSpec(memory_space=hbm)

        def pinned(x):
            return pltpu.with_memory_space_constraint(x, vmem)

        def shaped(x):
            return jax.ShapeDtypeStruct(x.shape, x.dtype)

        out_shape = (
            [vmem((n * depth, w), jnp.bfloat16) for w in widths]
            + [vmem((1, w), jnp.float32) for w in widths]
            + [vmem((n, wide, part // lanes, lanes), jnp.bfloat16)]
            + [vmem((depth, w), jnp.float32) for w in widths]
        )
        padded = sum(-(-w // 128) * 128 for w in widths)
        outside = padded * depth * (2 * n + 4) + (1 << 20)
        outs = pl.pallas_call(
            functools.partial(gather, n, wide, site, chunks),
            out_shape=out_shape,
            in_specs=[in_hbm] * 11,
            out_specs=[in_vmem] * 10,
            scratch_shapes=[vmem((depth, w), jnp.float32) for w in widths for _ in range(3)]
            + [
                vmem((2, part // lanes, lanes), jnp.float32),
                vmem((count, n, 1, 128), jnp.float32),
                dma((count, 3)),
                dma((2,)),
                dma((count, n)),
                dma((count, n)),
                dma((2, n - 1, count)),
                dma((2, n - 1, count)),
                dma,
                dma((n,)),
                dma((wide,)),
                dma((wide,)),
                vmem((head_of(depth, block_of(depth)), chunks[0][2]), jnp.float32),
                dma((3,)),
                dma((2,)),
                dma((2,)),
                vmem((part // lanes, lanes), jnp.bfloat16),
                dma((n,)),
                dma,
            ],
            compiler_params=pltpu.CompilerParams(
                collective_id=0,
                has_side_effects=True,
                vmem_limit_bytes=60 * (1 << 20) - outside,
            ),
        )(*arrays, *norms)
        outs = [pinned(x) for x in outs]
        stored = pl.pallas_call(
            functools.partial(store, n, site, kept),
            out_shape=[shaped(x) for x in outs] + [out_shape[3]],
            in_specs=[in_vmem] * 10,
            out_specs=[in_hbm] * 10 + [in_vmem],
            scratch_shapes=[dma((9 + 2 * n,))],
            compiler_params=pltpu.CompilerParams(vmem_limit_bytes=1 << 20),
        )(*outs)
        piece = pl.pallas_call(
            functools.partial(finish_gather, n, site),
            out_shape=vmem((depth, kept), jnp.bfloat16),
            in_specs=[in_vmem] * 2,
            out_specs=in_vmem,
            scratch_shapes=[dma((2,)), dma((2,))],
            compiler_params=pltpu.CompilerParams(
                collective_id=1, has_side_effects=True, vmem_limit_bytes=1 << 20
            ),
        )(outs[0], pinned(stored[10]))
        query = pl.pallas_call(
            functools.partial(finish_store, n, site),
            out_shape=shaped(stored[0]),
            in_specs=[in_hbm, in_vmem],
            out_specs=in_hbm,
            scratch_shapes=[pltpu.SemaphoreType.DMA],
            input_output_aliases={0: 0},
            compiler_params=pltpu.CompilerParams(vmem_limit_bytes=1 << 20),
        )(stored[0], pinned(piece))
        return (
            query,
            *stored[1:3],
            *(c.reshape(-1) for c in stored[3:6]),
            stored[6].reshape(-1),
            *stored[7:10],
        )

    cut = P(("site", "rows"), "width")
    return jax.shard_map(
        per_device,
        mesh=mesh,
        in_specs=(cut,) * 9 + (P(("site", "rows", "width")),) * 2,
        out_specs=(P("site", "width"),) * 3
        + (P(("site", "width")),) * 3
        + (P("site"),)
        + (cut,) * 3,
        check_vma=False,
    )
```
